256 devices in a mesh: gz: 16 (over z_hi, y, core), gy: 4 (over z_lo), ta: 4 (over x).
Axes of the slice: x: 4, y: 4, z: 8 (z_hi: 2, z_lo: 4; z = z_hi * 4 + z_lo), core: 2. Of those that a mesh axis runs over, the one named last changes fastest.
Arguments:
- movie: float32 [524288, 512], P(('gz', 'gy'), 'ta'), may hold values from 0 to 2
- traces: float32 [2048, 512], P(('gz', 'gy'), 'ta'), may hold values from 0.1 to 2
- entry_comp: int32 [4096, 8], P(('gz', 'gy')), may hold values from 0 to 2048, as said below
- footprints: float32 [4096, 8, 128], P(('gz', 'gy')), may hold values from 0.05 to 0.5
Outputs:
- traces_out: float32 [2048, 512], P(('gz', 'gy'), 'ta')
- footprints_out: float32 [4096, 8, 128], P(('gz', 'gy'))
The draws below stay inside these ranges and needn't reach their ends.
Inputs may be any that keep to these rules, and one draw needn't show every extreme that they name: `entry_comp`: the value 2048 marks an empty slot. In every tile the occupied slots come first; a tile holds up to 8 components, some tile holds 8 in every draw, and a component may appear in several tiles and blocks.
All inputs are finite; a program needn't handle non-finite values.
Results may differ from the reference program's by a relative error of at most 0.0001.
Values sent between devices are 32-bit elements; how exact they have to be, the bound alone decides.
No kernel may reach another device: no remote copies, remote signals or barrier semaphores. Data moves between devices by JAX's collectives and lax.ppermute only.
A program may use at most 64 MiB of HBM per device.

```python
import math
import jax
import jax.numpy as jnp
from jax import lax

K = 2048
TILE = 128
SLOTS_T = 8
TILES_DEV = 64
ITERS = 2
NTILES = 4096
VOXELS = 524288
FRAMES = 512


def draw_entry_comp(key, part):
    key_level = jax.random.fold_in(key, 11)
    key_count = jax.random.fold_in(key, 12)
    key_full = jax.random.fold_in(key, 13)
    key_comp = jax.random.fold_in(key, 14)
    blocks = NTILES // TILES_DEV
    level = jax.random.randint(key_level, (blocks,), 1, SLOTS_T + 1)
    tile_level = jnp.repeat(level, TILES_DEV, total_repeat_length=NTILES)
    counts = jax.random.randint(key_count, (NTILES,), 0, tile_level + 1)
    full_tile = jax.random.randint(key_full, (), 0, NTILES)
    counts = jnp.where(jnp.arange(NTILES) == full_tile, SLOTS_T, counts)
    comps = jax.random.randint(key_comp, (NTILES, SLOTS_T), 0, K)
    slot = jnp.arange(SLOTS_T)
    return jnp.where(slot[None, :] < counts[:, None], comps, K).astype(jnp.int32)


def block_levels(rng, shape, cuts, least, high):
    def one(axis_at, blocks):
        heights = jax.random.uniform(jax.random.fold_in(jax.random.fold_in(rng, 6), axis_at), (blocks,), jnp.float32, least / len(cuts), high / len(cuts))
        return jnp.repeat(jnp.exp(heights), shape[axis_at] // blocks).reshape((-1,) + (1,) * (len(shape) - axis_at - 1))

    gain = one(*cuts[0])
    for cut in cuts[1:]:
        gain = gain * one(*cut)
    return gain


def setup_inputs(seed: int = 0) -> dict:
    key_of = jax.random.split(jax.random.key(seed), 5)
    movie = jnp.clip(2.0 * jax.random.uniform(key_of[0], (VOXELS, FRAMES), jnp.float32) ** block_levels(key_of[0], (VOXELS, FRAMES), ((0, 64), (1, 4)), -0.2, 0.2), 0.0, 2.0)
    traces = jnp.clip(jnp.exp(math.log(2.0) - 2.9957323 * jax.random.uniform(key_of[1], (K, FRAMES), jnp.float32) ** block_levels(key_of[1], (K, FRAMES), ((0, 64), (1, 4)), -0.2, 0.2)), 0.1, 2.0)
    entry_comp = draw_entry_comp(jax.random.fold_in(key_of[4], 71), 0)
    footprints = jnp.clip(jnp.exp(math.log(0.5) - 2.3025851 * jax.random.uniform(key_of[3], (NTILES, SLOTS_T, TILE), jnp.float32) ** block_levels(key_of[3], (NTILES, SLOTS_T, TILE), ((0, 64),), -0.2, 0.2)), 0.05, 0.5)
    return dict(movie=movie, traces=traces, entry_comp=entry_comp, footprints=footprints)


RIDGE = 1.0


def pick_rows(traces_now, entry_comp):
    padded = jnp.concatenate([traces_now, jnp.zeros((1, traces_now.shape[1]), traces_now.dtype)], 0)
    return jnp.take(padded, entry_comp, axis=0)


def residual_of(tiles, foot, picked):
    recon = jnp.einsum("tjv,tjf->tvf", foot, picked, precision=lax.Precision.HIGHEST)
    return tiles - recon


def reference(movie, traces, entry_comp, footprints):
    ntiles = entry_comp.shape[0]
    frames = movie.shape[1]
    tiles = movie.reshape(ntiles, TILE, frames)
    valid = (entry_comp < K).astype(footprints.dtype)
    foot = footprints * valid[:, :, None]
    flat = entry_comp.reshape(-1)
    traces_now = traces
    for step in range(ITERS):
        picked = pick_rows(traces_now, entry_comp)
        resid = residual_of(tiles, foot, picked)
        cover = jnp.sum(foot, axis=1)
        proj = jnp.einsum("tjv,tvf->tjf", foot, resid, precision=lax.Precision.HIGHEST)
        curv = jnp.einsum("tjv,tv->tj", foot, cover, precision=lax.Precision.HIGHEST)
        numer = jax.ops.segment_sum(proj.reshape(-1, frames), flat, K + 1)[:K]
        denom = jax.ops.segment_sum(curv.reshape(-1), flat, K + 1)[:K]
        traces_now = jnp.maximum(traces_now + numer / (denom + RIDGE)[:, None], 0.0)
        picked = pick_rows(traces_now, entry_comp)
        resid = residual_of(tiles, foot, picked)
        grad = jnp.einsum("tvf,tjf->tjv", resid, picked, precision=lax.Precision.HIGHEST)
        gram = jnp.einsum("tjf,tif->tji", picked, picked, precision=lax.Precision.HIGHEST)
        dsp = jnp.sum(gram, axis=2) + RIDGE
        foot = jnp.maximum(foot + grad / dsp[:, :, None], 0.0) * valid[:, :, None]
    return traces_now, foot
```

```python
import jax
import jax.numpy as jnp
from jax import lax
from jax.experimental import pallas as pl
from jax.experimental.pallas import tpu as pltpu
from jax.sharding import Mesh
from jax.sharding import PartitionSpec as P

K = 2048
TILE = 128
SLOTS = 8
ITERS = 2
RIDGE = 1.0
BLOCKS = ("zh", "y", "c", "zl")
NGROUP = 4
GT = 16
HALF = 1024
NBLK = 16
ROWS = 72

VM = pl.BlockSpec(memory_space=pltpu.VMEM)
PARAMS = pltpu.CompilerParams(vmem_limit_bytes=24 * 1024 * 1024)
f32 = jnp.float32
bf16 = jnp.bfloat16


def split(x):
    hi = x.astype(bf16)
    lo = (x - hi.astype(f32)).astype(bf16)
    return hi, lo


def nt(a, b):
    return lax.dot_general(a, b, (((1,), (1,)), ((), ())), preferred_element_type=f32)


def nn(a, b):
    return lax.dot_general(a, b, (((1,), (0,)), ((), ())), preferred_element_type=f32)


def nt3(a, b):
    ah, al = split(a)
    bh, bl = split(b)
    return nt(ah, bh) + (nt(ah, bl) + nt(al, bh))


def nn3(a, b):
    ah, al = split(a)
    bh, bl = split(b)
    return nn(ah, bh) + (nn(ah, bl) + nn(al, bh))


def same_tile():
    i = lax.broadcasted_iota(jnp.int32, (128, 128), 0) // SLOTS
    j = lax.broadcasted_iota(jnp.int32, (128, 128), 1) // SLOTS
    return i == j


def stacked(x):
    hi = x.astype(bf16).astype(f32)
    return jnp.concatenate([hi, x - hi], axis=0).astype(bf16)


def as_column(row, n):
    i = lax.broadcasted_iota(jnp.int32, (n, n), 0)
    j = lax.broadcasted_iota(jnp.int32, (n, n), 1)
    return jnp.sum(jnp.where(i == j, row, 0.0), axis=1, keepdims=True)


def project(foot, pair):
    two = stacked(foot)
    out = nn(jnp.concatenate([two, two], axis=1), pair)
    return out[:SLOTS] + out[SLOTS:]


def correlate(picked, pair):
    out = nt(stacked(picked), pair)
    out = out[:SLOTS] + out[SLOTS:]
    return out[:, :TILE] + out[:, TILE:]


def first_kernel(movie, foot, pairs, proj, gram):
    f = foot[...]
    gram[0] = jnp.where(same_tile(), nt3(f, f), 0.0)
    for t in range(GT):
        hi, lo = split(movie[t * TILE : (t + 1) * TILE, :])
        pairs[t, :TILE, :] = hi
        pairs[t, TILE:, :] = lo
    for t in range(GT):
        rows = slice(t * SLOTS, (t + 1) * SLOTS)
        proj[rows, :] = project(foot[rows, :], pairs[t])


def first(movie, foot):
    return pl.pallas_call(
        first_kernel,
        grid=(NGROUP,),
        in_specs=[
            pl.BlockSpec((GT * TILE, 128), lambda g: (g, 0)),
            pl.BlockSpec((128, TILE), lambda g: (g, 0)),
        ],
        out_specs=[
            pl.BlockSpec((GT, 2 * TILE, 128), lambda g: (g, 0, 0)),
            pl.BlockSpec((128, 128), lambda g: (g, 0)),
            pl.BlockSpec((1, 128, 128), lambda g: (g, 0, 0)),
        ],
        out_shape=[
            jax.ShapeDtypeStruct((NGROUP * GT, 2 * TILE, 128), bf16),
            jax.ShapeDtypeStruct((NGROUP * 128, 128), f32),
            jax.ShapeDtypeStruct((NGROUP, 128, 128), f32),
        ],
        compiler_params=PARAMS,
        name="first",
    )(movie, foot)


def scatter(place, values, curv, mine, other):
    hi, lo = split(values)
    both = jnp.concatenate([hi, lo], axis=1)
    n = place.shape[1]
    lane = lax.broadcasted_iota(jnp.int32, (128, n), 0)
    inside = jnp.where(lane == place % 64, 1.0, 0.0).astype(bf16)
    block = lax.broadcasted_iota(jnp.int32, (2 * NBLK, n), 0)
    ch, cl = split(jnp.where(block == place // 64, curv, 0.0))
    den = nt(ch, inside) + nt(cl, inside)
    for half, out in ((0, mine), (1, other)):
        for b in range(0, NBLK, 2):
            base = half * HALF + b * 64
            hot = jnp.where(lane + base == place, 1.0, 0.0).astype(bf16)
            got = nn(hot, both)
            got = got[:, :128] + got[:, 128:]
            for q in range(2):
                out[b + q, :64, :] = got[q * 64 : (q + 1) * 64]
                row = half * NBLK + b + q
                out[b + q, 64:, :] = jnp.broadcast_to(den[row : row + 1], (8, 128))


def numer_kernel(place, proj, gram, picked, mine, other, work):
    rows = []
    for g in range(NGROUP):
        s = slice(g * 128, (g + 1) * 128)
        work[s, :] = proj[s, :] - nn3(gram[g], picked[s, :])
        rows.append(jnp.sum(gram[g], axis=0, keepdims=True))
    scatter(place[...], work[...], jnp.concatenate(rows, axis=1), mine, other)


def numer_out():
    return [jax.ShapeDtypeStruct((NBLK, ROWS, 128), f32)] * 2


def numerators(place, proj, gram, picked):
    return pl.pallas_call(
        numer_kernel,
        in_specs=[VM] * 4,
        out_specs=[VM] * 2,
        out_shape=numer_out(),
        scratch_shapes=[pltpu.VMEM((512, 128), f32)],
        compiler_params=PARAMS,
        name="numerators",
    )(place, proj, gram, picked)


def update_kernel(own, came, traces, out, wide):
    total = own[...] + came[...]
    den = jnp.concatenate([total[64:65, :]], axis=0)
    col = as_column(den, 128)[:64]
    new = jnp.maximum(traces[...] + total[:64] / (col + RIDGE), 0.0)
    out[...] = new
    for b in range(NBLK):
        wide[b] = new


def update(own, came, traces):
    return pl.pallas_call(
        update_kernel,
        in_specs=[VM] * 3,
        out_specs=[VM] * 2,
        out_shape=[
            jax.ShapeDtypeStruct((64, 128), f32),
            jax.ShapeDtypeStruct((NBLK, 64, 128), f32),
        ],
        compiler_params=PARAMS,
        name="update",
    )(own, came, traces)


def grad_kernel(picked, foot, pairs, out):
    for g in range(NGROUP):
        s = slice(g * 128, (g + 1) * 128)
        p = picked[s, :]
        gram = jnp.where(same_tile(), nt3(p, p), 0.0)
        out[g, :128, :] = -nn3(gram, foot[s, :])
        out[g, 128:, :] = jnp.broadcast_to(jnp.sum(gram, axis=0, keepdims=True), (8, 128))
        for t in range(GT):
            rows = slice(t * SLOTS, (t + 1) * SLOTS)
            at = slice(g * 128 + t * SLOTS, g * 128 + (t + 1) * SLOTS)
            out[g, rows, :] += correlate(picked[at, :], pairs[g * GT + t])


def gradients(picked, foot, pairs):
    return pl.pallas_call(
        grad_kernel,
        in_specs=[VM] * 3,
        out_specs=VM,
        out_shape=jax.ShapeDtypeStruct((NGROUP, 136, 128), f32),
        compiler_params=PARAMS,
        name="gradients",
    )(picked, foot, pairs)


def stepped(g, parts, foot, valid):
    a, b, c, d = (x[g] for x in parts)
    total = (a + b) + (c + d)
    dsp = as_column(total[128:129, :], 128) + RIDGE
    s = slice(g * 128, (g + 1) * 128)
    return jnp.maximum(foot[s, :] + total[:128] / dsp, 0.0) * valid[s, :]


def middle_kernel(place, a, b, c, d, foot, valid, picked, pairs, new, mine, other, work):
    rows = []
    for g in range(NGROUP):
        s = slice(g * 128, (g + 1) * 128)
        f = stepped(g, (a, b, c, d), foot, valid)
        new[s, :] = f
        gram = jnp.where(same_tile(), nt3(f, f), 0.0)
        rows.append(jnp.sum(gram, axis=0, keepdims=True))
        work[s, :] = -nn3(gram, picked[s, :])
        for t in range(GT):
            at = slice(g * 128 + t * SLOTS, g * 128 + (t + 1) * SLOTS)
            work[at, :] += project(f[t * SLOTS : (t + 1) * SLOTS], pairs[g * GT + t])
    scatter(place[...], work[...], jnp.concatenate(rows, axis=1), mine, other)


def middle(place, parts, foot, valid, picked, pairs):
    return pl.pallas_call(
        middle_kernel,
        in_specs=[VM] * 9,
        out_specs=[VM] * 3,
        out_shape=[jax.ShapeDtypeStruct((512, TILE), f32)] + numer_out(),
        scratch_shapes=[pltpu.VMEM((512, 128), f32)],
        compiler_params=PARAMS,
        name="middle",
    )(place, *parts, foot, valid, picked, pairs)


def last_kernel(a, b, c, d, foot, valid, new):
    for g in range(NGROUP):
        new[g * 128 : (g + 1) * 128, :] = stepped(g, (a, b, c, d), foot, valid)


def last(parts, foot, valid):
    return pl.pallas_call(
        last_kernel,
        in_specs=[VM] * 6,
        out_specs=VM,
        out_shape=jax.ShapeDtypeStruct((512, TILE), f32),
        compiler_params=PARAMS,
        name="last",
    )(*parts, foot, valid)


def swapped(x, axis):
    n = lax.axis_size(axis)
    return lax.ppermute(x, axis, [(i, i ^ 1) for i in range(n)])


def summed_blocks(mine, other):
    mine = mine + swapped(other, "c")
    came = lax.all_to_all(mine, ("y", "zl"), 0, 0, tiled=True)
    own = came.sum(axis=0)
    return own, swapped(own, "zh")


def spread(wide):
    mine = lax.all_to_all(wide, ("y", "zl"), 0, 0, tiled=True).reshape(HALF, 128)
    return mine, swapped(mine, "c")


def over_frames(x):
    one, two, three = (
        lax.ppermute(x, "ta", [(i, i ^ k) for i in range(4)]) for k in (1, 2, 3)
    )
    return x, one, two, three


def pick(halves, index):
    zero = jnp.zeros((8, 128), f32)
    whole = jnp.concatenate([*halves, zero], axis=0)
    return whole.at[index].get(mode="promise_in_bounds")


def local(movie, traces, entry_comp, footprints):
    core = lax.axis_index("c")
    owner = entry_comp // 32
    zh, y, c, zl = owner // 32, (owner // 8) % 4, (owner // 4) % 2, owner % 4
    index = ((c ^ core) * HALF + ((y * 4 + zl) * 2 + zh) * 32 + entry_comp % 32).reshape(-1)
    occupied = entry_comp.reshape(-1) < K
    index = jnp.where(occupied, index, K)
    place = index[None, :]
    valid = occupied.astype(f32)[:, None]
    foot = footprints.reshape(-1, TILE) * valid

    tiles = jnp.broadcast_to(traces[None], (32, 32, 128))
    mine = lax.all_to_all(tiles, ("y", "zl", "zh"), 0, 0, tiled=True).reshape(HALF, 128)
    halves = (mine, swapped(mine, "c"))
    pairs, proj, gram = first(movie, foot)
    at = (lax.axis_index("y") * 4 + lax.axis_index("zl")) * 64
    block = lax.dynamic_slice_in_dim(mine, at, 64, 0)
    picked = pick(halves, index)
    sums = numerators(place, proj, gram, picked)
    for step in range(ITERS):
        block, wide = update(*summed_blocks(*sums), block)
        picked = pick(spread(wide), index)
        parts = over_frames(gradients(picked, foot, pairs))
        if step + 1 < ITERS:
            foot, *sums = middle(place, parts, foot, valid, picked, pairs)
        else:
            foot = last(parts, foot, valid)
    out = lax.dynamic_slice_in_dim(block, lax.axis_index("zh") * 32, 32, 0)
    return out, foot.reshape(footprints.shape)


def solution(mesh):
    torus = Mesh(
        mesh.devices.reshape(2, 4, 2, mesh.shape["gy"], mesh.shape["ta"]),
        ("zh", "y", "c", "zl", "ta"),
    )
    in_specs = (P(BLOCKS, "ta"), P(BLOCKS, "ta"), P(BLOCKS, None), P(BLOCKS, None, None))
    out_specs = (P(BLOCKS, "ta"), P(BLOCKS, None, None))
    return jax.shard_map(local, mesh=torus, in_specs=in_specs, out_specs=out_specs, check_vma=False)
```

```python
import jax
import jax.numpy as jnp
from jax import lax
from jax.experimental import pallas as pl
from jax.experimental.pallas import tpu as pltpu
from jax.sharding import Mesh
from jax.sharding import PartitionSpec as P

K = 2048
TILE = 128
SLOTS = 8
ITERS = 2
RIDGE = 1.0
BLOCKS = ("zh", "y", "c", "zl")
NGROUP = 4
GT = 16
HALF = 1024
NBLK = 16
ROWS = 72

VM = pl.BlockSpec(memory_space=pltpu.VMEM)
SM = pl.BlockSpec(memory_space=pltpu.SMEM)
HB = pl.BlockSpec(memory_space=pltpu.HBM)
PARAMS = pltpu.CompilerParams(vmem_limit_bytes=24 * 1024 * 1024)
f32 = jnp.float32
bf16 = jnp.bfloat16


def like(*shape, dtype=f32):
    return jax.ShapeDtypeStruct(shape, dtype)


def split(x):
    hi = x.astype(bf16)
    lo = (x - hi.astype(f32)).astype(bf16)
    return hi, lo


def nt(a, b):
    return lax.dot_general(a, b, (((1,), (1,)), ((), ())), preferred_element_type=f32)


def nn(a, b):
    return lax.dot_general(a, b, (((1,), (0,)), ((), ())), preferred_element_type=f32)


def nt3(a, b):
    ah, al = split(a)
    bh, bl = split(b)
    return nt(ah, bh) + (nt(ah, bl) + nt(al, bh))


def nn3(a, b):
    ah, al = split(a)
    bh, bl = split(b)
    return nn(ah, bh) + (nn(ah, bl) + nn(al, bh))


def same_tile():
    i = lax.broadcasted_iota(jnp.int32, (128, 128), 0) // SLOTS
    j = lax.broadcasted_iota(jnp.int32, (128, 128), 1) // SLOTS
    return i == j


def stacked(x):
    hi = x.astype(bf16).astype(f32)
    return jnp.concatenate([hi, x - hi], axis=0).astype(bf16)


def as_column(row, n):
    i = lax.broadcasted_iota(jnp.int32, (n, n), 0)
    j = lax.broadcasted_iota(jnp.int32, (n, n), 1)
    return jnp.sum(jnp.where(i == j, row, 0.0), axis=1, keepdims=True)


def project(foot, pair):
    two = stacked(foot)
    out = nn(jnp.concatenate([two, two], axis=1), pair)
    return out[:SLOTS] + out[SLOTS:]


def correlate(picked, pair):
    out = nt(stacked(picked), pair)
    out = out[:SLOTS] + out[SLOTS:]
    return out[:, :TILE] + out[:, TILE:]


def rows_of(g):
    return pl.ds(pl.multiple_of(g * 128, 128), 128)


def tiles_of(g):
    return pl.ds(pl.multiple_of(g * GT, GT), GT)


def turned(x, k):
    return (x + k) % NGROUP


def first_kernel(movie, foot, pairs, proj, gram, frames, held, came, sent):
    loads = []
    for g in range(NGROUP):
        at = pl.ds(g * GT * TILE, GT * TILE)
        loads.append(pltpu.make_async_copy(movie.at[at], frames.at[at], came.at[g]))
        loads[-1].start()
    stores = []
    for g in range(NGROUP):
        s = slice(g * 128, (g + 1) * 128)
        f = foot[s, :]
        gram[g] = jnp.where(same_tile(), nt3(f, f), 0.0)
        loads[g].wait()
        for t in range(g * GT, (g + 1) * GT):
            hi, lo = split(frames[t * TILE : (t + 1) * TILE, :])
            held[t, :TILE, :] = hi
            held[t, TILE:, :] = lo
        at = pl.ds(g * GT, GT)
        stores.append(pltpu.make_async_copy(held.at[at], pairs.at[at], sent.at[g]))
        stores[-1].start()
        for t in range(g * GT, (g + 1) * GT):
            rows = slice(t * SLOTS, (t + 1) * SLOTS)
            proj[rows, :] = project(foot[rows, :], held[t])
    for g in range(NGROUP):
        stores[g].wait()


def first(movie, foot):
    return pl.pallas_call(
        first_kernel,
        in_specs=[HB, VM],
        out_specs=[HB, VM, VM],
        out_shape=[like(64, 2 * TILE, 128, dtype=bf16), like(512, 128), like(NGROUP, 128, 128)],
        scratch_shapes=[
            pltpu.VMEM((64 * TILE, 128), f32),
            pltpu.VMEM((64, 2 * TILE, 128), bf16),
            pltpu.SemaphoreType.DMA((NGROUP,)),
            pltpu.SemaphoreType.DMA((NGROUP,)),
        ],
        compiler_params=PARAMS,
        name="first",
    )(movie, foot)


def scatter(place, values, curv, mine, other):
    hi, lo = split(values)
    both = jnp.concatenate([hi, lo], axis=1)
    n = place.shape[1]
    lane = lax.broadcasted_iota(jnp.int32, (128, n), 0)
    inside = jnp.where(lane == place % 64, 1.0, 0.0).astype(bf16)
    block = lax.broadcasted_iota(jnp.int32, (2 * NBLK, n), 0)
    ch, cl = split(jnp.where(block == place // 64, curv, 0.0))
    den = nt(ch, inside) + nt(cl, inside)
    for half, out in ((0, mine), (1, other)):
        for b in range(0, NBLK, 2):
            base = half * HALF + b * 64
            hot = jnp.where(lane + base == place, 1.0, 0.0).astype(bf16)
            got = nn(hot, both)
            got = got[:, :128] + got[:, 128:]
            for q in range(2):
                out[b + q, :64, :] = got[q * 64 : (q + 1) * 64]
                row = half * NBLK + b + q
                out[b + q, 64:, :] = jnp.broadcast_to(den[row : row + 1], (8, 128))


def halved(mine, other, table):
    for half, part in ((0, mine), (1, other)):
        hi, lo = split(part[...])
        table[half * HALF : (half + 1) * HALF, :128] = hi
        table[half * HALF : (half + 1) * HALF, 128:] = lo


def picked_rows(place, table):
    lane = lax.broadcasted_iota(jnp.int32, (128, K), 1)
    hot = jnp.where(lane == place, 1.0, 0.0).astype(bf16)
    got = nn(hot, table[...])
    return got[:, :128] + got[:, 128:]


def sums_out():
    return [like(NBLK, ROWS, 128)] * 2


TABLE = pltpu.VMEM((K, 256), bf16)
SLOTS_BY_FRAMES = pltpu.VMEM((512, 128), f32)


def numer_kernel(place, column, proj, gram, near, far, mine, other, work, table):
    halved(near, far, table)
    rows = []
    for g in range(NGROUP):
        s = slice(g * 128, (g + 1) * 128)
        picked = picked_rows(column[s, :], table)
        work[s, :] = proj[s, :] - nn3(gram[g], picked)
        rows.append(jnp.sum(gram[g], axis=0, keepdims=True))
    scatter(place[...], work[...], jnp.concatenate(rows, axis=1), mine, other)


def numerators(place, column, proj, gram, halves):
    return pl.pallas_call(
        numer_kernel,
        in_specs=[VM] * 6,
        out_specs=[VM] * 2,
        out_shape=sums_out(),
        scratch_shapes=[SLOTS_BY_FRAMES, TABLE],
        compiler_params=PARAMS,
        name="numerators",
    )(place, column, proj, gram, *halves)


def fold_core_kernel(mine, came, *outs):
    for k in range(4):
        for q in range(4):
            outs[k][q] = mine[k * 4 + q] + came[k * 4 + q]


def fold_core(mine, came):
    return pl.pallas_call(
        fold_core_kernel,
        in_specs=[VM] * 2,
        out_specs=[VM] * 4,
        out_shape=[like(4, ROWS, 128)] * 4,
        compiler_params=PARAMS,
        name="fold_core",
    )(mine, came)


def fold_y_kernel(a, b, c, d, *outs):
    for k in range(4):
        outs[k][...] = (a[k] + b[k]) + (c[k] + d[k])


def fold_y(parts):
    return pl.pallas_call(
        fold_y_kernel,
        in_specs=[VM] * 4,
        out_specs=[VM] * 4,
        out_shape=[like(ROWS, 128)] * 4,
        compiler_params=PARAMS,
        name="fold_y",
    )(*parts)


def fold_z_kernel(a, b, c, d, out):
    out[...] = (a[...] + b[...]) + (c[...] + d[...])


def fold_z(parts):
    return pl.pallas_call(
        fold_z_kernel,
        in_specs=[VM] * 4,
        out_specs=VM,
        out_shape=like(ROWS, 128),
        compiler_params=PARAMS,
        name="fold_z",
    )(*parts)


def update_kernel(own, came, traces, out):
    a = as_column(own[64:65, :], 128)
    b = as_column(came[64:65, :], 128)
    for h in range(2):
        s = slice(h * 32, (h + 1) * 32)
        o = slice((1 - h) * 32, (2 - h) * 32)
        den = a[s] + b[o] + RIDGE
        out[s, :] = jnp.maximum(traces[s, :] + (own[s, :] + came[o, :]) / den, 0.0)


def update(own, came, traces):
    return pl.pallas_call(
        update_kernel,
        in_specs=[VM] * 3,
        out_specs=VM,
        out_shape=like(64, 128),
        compiler_params=PARAMS,
        name="update",
    )(own, came, traces)


def fetch(pairs, held, arrived, order):
    copies = []
    for k, g in enumerate(order):
        copies.append(
            pltpu.make_async_copy(pairs.at[tiles_of(g)], held.at[k], arrived.at[k])
        )
        copies[-1].start()
    return copies


PAIRS = pltpu.VMEM((NGROUP, GT, 2 * TILE, 128), bf16)
ARRIVED = pltpu.SemaphoreType.DMA((NGROUP,))


def grad_kernel(me, column, near, far, foot, pairs, picked, o0, o1, o2, o3, table, held, arrived):
    order = [turned(me[0], k) for k in range(NGROUP)]
    copies = fetch(pairs, held, arrived, order)
    halved(near, far, table)
    for k, out in enumerate((o0, o1, o2, o3)):
        s = rows_of(order[k])
        p = picked_rows(column[s, :], table)
        picked[s, :] = p
        gram = jnp.where(same_tile(), nt3(p, p), 0.0)
        out[128:, :] = jnp.broadcast_to(jnp.sum(gram, axis=0, keepdims=True), (8, 128))
        less = nn3(gram, foot[s, :])
        copies[k].wait()
        for t in range(GT):
            rows = slice(t * SLOTS, (t + 1) * SLOTS)
            out[rows, :] = correlate(p[rows], held[k, t]) - less[rows]


def gradients(me, column, halves, foot, pairs):
    return pl.pallas_call(
        grad_kernel,
        in_specs=[SM, VM, VM, VM, VM, HB],
        out_specs=[VM] * 5,
        out_shape=[like(512, 128)] + [like(136, 128)] * 4,
        scratch_shapes=[TABLE, PAIRS, ARRIVED],
        compiler_params=PARAMS,
        name="gradients",
    )(me, column, *halves, foot, pairs)


def step_kernel(me, a, b, c, d, foot, valid, new):
    total = (a[...] + b[...]) + (c[...] + d[...])
    dsp = as_column(total[128:129, :], 128) + RIDGE
    s = rows_of(me[0])
    new[...] = jnp.maximum(foot[s, :] + total[:128] / dsp, 0.0) * valid[s, :]


def stepped(me, parts, foot, valid):
    return pl.pallas_call(
        step_kernel,
        in_specs=[SM] + [VM] * 6,
        out_specs=VM,
        out_shape=like(128, TILE),
        compiler_params=PARAMS,
        name="step",
    )(me, *parts, foot, valid)


def middle_kernel(
    me, place, f0, f1, f2, f3, picked, pairs, new, mine, other, work, curv, held, arrived
):
    order = [turned(me[0], k) for k in range(NGROUP)]
    copies = fetch(pairs, held, arrived, order)
    for k, foot in enumerate((f0, f1, f2, f3)):
        s = rows_of(order[k])
        f = foot[...]
        new[s, :] = f
        gram = jnp.where(same_tile(), nt3(f, f), 0.0)
        curv[order[k]] = jnp.broadcast_to(jnp.sum(gram, axis=0, keepdims=True), (8, 128))
        less = nn3(gram, picked[s, :])
        copies[k].wait()
        parts = []
        for t in range(GT):
            parts.append(project(f[t * SLOTS : (t + 1) * SLOTS], held[k, t]))
        work[s, :] = jnp.concatenate(parts, axis=0) - less
    row = jnp.concatenate([curv[g, :1, :] for g in range(NGROUP)], axis=1)
    scatter(place[...], work[...], row, mine, other)


def middle(me, place, feet, picked, pairs):
    return pl.pallas_call(
        middle_kernel,
        in_specs=[SM] + [VM] * 6 + [HB],
        out_specs=[VM] * 3,
        out_shape=[like(512, TILE)] + sums_out(),
        scratch_shapes=[SLOTS_BY_FRAMES, pltpu.VMEM((NGROUP, 8, 128), f32), PAIRS, ARRIVED],
        compiler_params=PARAMS,
        name="middle",
    )(me, place, *feet, picked, pairs)


def last_kernel(me, f0, f1, f2, f3, new):
    for k, foot in enumerate((f0, f1, f2, f3)):
        new[rows_of(turned(me[0], k)), :] = foot[...]


def last(me, feet):
    return pl.pallas_call(
        last_kernel,
        in_specs=[SM] + [VM] * 4,
        out_specs=VM,
        out_shape=like(512, TILE),
        compiler_params=PARAMS,
        name="last",
    )(me, *feet)


def moved(x, axis, k):
    n = lax.axis_size(axis)
    return lax.ppermute(x, axis, [(i, (i + k) % n) for i in range(n)])


def swapped(x, axis, bits):
    n = lax.axis_size(axis)
    return lax.ppermute(x, axis, [(i, i ^ bits) for i in range(n)])


def across(x):
    return swapped(x, ("zh", "zl"), 7)


def summed_blocks(mine, other):
    ys = fold_core(mine, swapped(other, "c", 1))
    zs = fold_y([ys[0]] + [moved(ys[k], "y", k) for k in (1, 2, 3)])
    own = fold_z([zs[0]] + [swapped(zs[k], "zl", k) for k in (1, 2, 3)])
    return own, across(own)


def spread(block):
    mine = jnp.concatenate([block] + [swapped(block, "zl", k) for k in (1, 2, 3)], axis=0)
    mine = jnp.concatenate([mine] + [moved(mine, "y", -k) for k in (1, 2, 3)], axis=0)
    return mine, swapped(mine, "c", 1)


def over_frames(me, pieces, foot, valid):
    parts = [pieces[0]] + [moved(pieces[k], "ta", k) for k in (1, 2, 3)]
    own = stepped(me, parts, foot, valid)
    return [own] + [moved(own, "ta", -k) for k in (1, 2, 3)]


def local(movie, traces, entry_comp, footprints):
    me = lax.axis_index("ta").astype(jnp.int32).reshape(1)
    zh, y, c, zl = (lax.axis_index(name) for name in BLOCKS)
    owner = entry_comp // 32
    ozh, oy, oc, ozl = owner // 32, (owner // 8) % 4, (owner // 4) % 2, owner % 4
    block = ((oc ^ c) * 4 + (oy - y) % 4) * 4 + (ozl ^ (3 * ozh) ^ zl ^ (3 * zh))
    index = (block * 64 + (ozh ^ zh) * 32 + entry_comp % 32).reshape(-1)
    occupied = entry_comp.reshape(-1) < K
    index = jnp.where(occupied, index, K)
    place, column = index[None, :], index[:, None]
    valid = occupied.astype(f32)[:, None]
    foot = footprints.reshape(-1, TILE) * valid

    own = jnp.concatenate([traces, across(traces)], axis=0)
    pairs, proj, gram = first(movie, foot)
    sums = numerators(place, column, proj, gram, spread(own))
    for step in range(ITERS):
        own = update(*summed_blocks(*sums), own)
        picked, *pieces = gradients(me, column, spread(own), foot, pairs)
        feet = over_frames(me, pieces, foot, valid)
        if step + 1 < ITERS:
            foot, *sums = middle(me, place, feet, picked, pairs)
        else:
            foot = last(me, feet)
    return own[:32], foot.reshape(footprints.shape)


def solution(mesh):
    torus = Mesh(
        mesh.devices.reshape(2, 4, 2, mesh.shape["gy"], mesh.shape["ta"]),
        ("zh", "y", "c", "zl", "ta"),
    )
    in_specs = (P(BLOCKS, "ta"), P(BLOCKS, "ta"), P(BLOCKS, None), P(BLOCKS, None, None))
    out_specs = (P(BLOCKS, "ta"), P(BLOCKS, None, None))
    return jax.shard_map(local, mesh=torus, in_specs=in_specs, out_specs=out_specs, check_vma=False)
```

```python
import jax
import jax.numpy as jnp
from jax import lax
from jax.experimental import pallas as pl
from jax.experimental.pallas import tpu as pltpu
from jax.sharding import Mesh
from jax.sharding import PartitionSpec as P

K = 2048
TILE = 128
SLOTS = 8
ITERS = 2
RIDGE = 1.0
BLOCKS = ("zh", "y", "c", "zl")
NGROUP = 4
GT = 16
HALF = 1024
NBLK = 16
ROWS = 72

VM = pl.BlockSpec(memory_space=pltpu.VMEM)
HB = pl.BlockSpec(memory_space=pltpu.HBM)
PARAMS = pltpu.CompilerParams(vmem_limit_bytes=24 * 1024 * 1024)
f32 = jnp.float32
bf16 = jnp.bfloat16


def like(*shape, dtype=f32):
    return jax.ShapeDtypeStruct(shape, dtype)


def cost(macs):
    return pl.CostEstimate(flops=2 * macs, bytes_accessed=1 << 20, transcendentals=0)


def split(x):
    hi = x.astype(bf16)
    lo = (x - hi.astype(f32)).astype(bf16)
    return hi, lo


def nt(a, b):
    return lax.dot_general(a, b, (((1,), (1,)), ((), ())), preferred_element_type=f32)


def nn(a, b):
    return lax.dot_general(a, b, (((1,), (0,)), ((), ())), preferred_element_type=f32)


def nt3(a, b):
    ah, al = split(a)
    bh, bl = split(b)
    return nt(ah, bh) + (nt(ah, bl) + nt(al, bh))


def nn3(a, b):
    ah, al = split(a)
    bh, bl = split(b)
    return nn(ah, bh) + (nn(ah, bl) + nn(al, bh))


def same_tile():
    i = lax.broadcasted_iota(jnp.int32, (128, 128), 0) // SLOTS
    j = lax.broadcasted_iota(jnp.int32, (128, 128), 1) // SLOTS
    return i == j


def stacked(x):
    hi = x.astype(bf16).astype(f32)
    return jnp.concatenate([hi, x - hi], axis=0).astype(bf16)


def as_column(row, n):
    i = lax.broadcasted_iota(jnp.int32, (n, n), 0)
    j = lax.broadcasted_iota(jnp.int32, (n, n), 1)
    return jnp.sum(jnp.where(i == j, row, 0.0), axis=1, keepdims=True)


def project(foot, pair):
    two = stacked(foot)
    out = nn(jnp.concatenate([two, two], axis=1), pair)
    return out[:SLOTS] + out[SLOTS:]


def correlate(picked, pair):
    out = nt(stacked(picked), pair)
    out = out[:SLOTS] + out[SLOTS:]
    return out[:, :TILE] + out[:, TILE:]


def rows_of(g):
    return pl.ds(pl.multiple_of(g * 128, 128), 128)


def prepare_kernel(place, footprints, column, valid, foot):
    for g in range(NGROUP):
        s = rows_of(g)
        row = place[:, g * 128 : (g + 1) * 128].astype(f32)
        at = as_column(row, 128)
        column[s, :] = at.astype(jnp.int32)
        valid[s, :] = jnp.where(at < K, 1.0, 0.0)
        foot[s, :] = footprints[s, :] * jnp.where(at < K, 1.0, 0.0)


def prepare(place, footprints):
    return pl.pallas_call(
        prepare_kernel,
        in_specs=[VM] * 2,
        out_specs=[VM] * 3,
        out_shape=[like(512, 1, dtype=jnp.int32), like(512, 1), like(512, TILE)],
        compiler_params=PARAMS,
        name="prepare",
    )(place, footprints)


def first_kernel(movie, foot, pairs, proj, gram, frames, came):
    for g in range(NGROUP):
        at = pl.ds(g * GT * TILE, GT * TILE)
        pltpu.make_async_copy(movie.at[at], frames.at[at], came.at[g]).start()

    def group(g, carry):
        at = pl.ds(pl.multiple_of(g * GT * TILE, GT * TILE), GT * TILE)
        pltpu.make_async_copy(movie.at[at], frames.at[at], came.at[g]).wait()
        f = foot[rows_of(g), :]
        gram[g] = jnp.where(same_tile(), nt3(f, f), 0.0)
        parts = []
        for t in range(GT):
            at = pl.ds(pl.multiple_of((g * GT + t) * TILE, TILE), TILE)
            hi, lo = split(frames[at, :])
            pair = jnp.concatenate([hi, lo], axis=0)
            pairs[g * GT + t] = pair
            parts.append(project(f[t * SLOTS : (t + 1) * SLOTS], pair))
        proj[rows_of(g), :] = jnp.concatenate(parts, axis=0)
        return carry

    lax.fori_loop(0, NGROUP, group, 0)


def first(movie, foot):
    return pl.pallas_call(
        first_kernel,
        in_specs=[HB, VM],
        out_specs=[VM, VM, VM],
        out_shape=[pltpu.VMEM((64, 2 * TILE, 128), bf16), like(512, 128), like(NGROUP, 128, 128)],
        scratch_shapes=[pltpu.VMEM((64 * TILE, 128), f32), pltpu.SemaphoreType.DMA((NGROUP,))],
        compiler_params=PARAMS,
        cost_estimate=cost(64 * 16 * 256 * 128),
        name="first",
    )(pltpu.with_memory_space_constraint(movie, pltpu.HBM), foot)


def scatter(half, place, both, curv, out):
    n = place.shape[1]
    lane = lax.broadcasted_iota(jnp.int32, (256, n), 0)
    inside = jnp.where(lane[:128] == place % 64, 1.0, 0.0).astype(bf16)
    block = lax.broadcasted_iota(jnp.int32, (NBLK, n), 0) + half * NBLK
    ch, cl = split(jnp.where(block == place // 64, curv, 0.0))
    den = nt(ch, inside) + nt(cl, inside)
    for b in range(0, NBLK, 4):
        hot = jnp.where(lane + (half * HALF + b * 64) == place, 1.0, 0.0).astype(bf16)
        got = nn(hot, both)
        got = got[:, :128] + got[:, 128:]
        for q in range(4):
            out[b + q, :64, :] = got[q * 64 : (q + 1) * 64]
            out[b + q, 64:, :] = jnp.broadcast_to(den[b + q : b + q + 1], (8, 128))


def picked_from(half, column, part):
    both = jnp.concatenate(split(part), axis=1)
    lane = lax.broadcasted_iota(jnp.int32, (512, HALF), 1) + half * HALF
    hot = jnp.where(lane == column, 1.0, 0.0).astype(bf16)
    got = nn(hot, both)
    return got[:, :128] + got[:, 128:]


def near_kernel(column, near, out):
    out[...] = picked_from(0, column[...], near[...])


def pick_near(column, near):
    return pl.pallas_call(
        near_kernel,
        in_specs=[VM] * 2,
        out_specs=VM,
        out_shape=like(512, 128),
        compiler_params=PARAMS,
        cost_estimate=cost(512 * HALF * 256),
        name="pick_near",
    )(column, near)


SLOTS_BY_FRAMES = pltpu.VMEM((512, 128), f32)
FAR_OUT = [like(NBLK, ROWS, 128), like(512, 256, dtype=bf16), like(8, 512)]


def scatter_far(place, work, rows, other, both, curv):
    two = jnp.concatenate(split(work[...]), axis=1)
    row = jnp.concatenate(rows, axis=1)
    both[...] = two
    curv[...] = jnp.broadcast_to(row, (8, 512))
    scatter(1, place[...], two, row, other)


def numer_kernel(place, column, proj, gram, got, far, other, both, curv, work):
    work[...] = got[...] + picked_from(1, column[...], far[...])
    rows = []
    for g in range(NGROUP):
        s = slice(g * 128, (g + 1) * 128)
        work[s, :] = proj[s, :] - nn3(gram[g], work[s, :])
        rows.append(jnp.sum(gram[g], axis=0, keepdims=True))
    scatter_far(place, work, rows, other, both, curv)


def numerators(place, column, proj, gram, got, far):
    return pl.pallas_call(
        numer_kernel,
        in_specs=[VM] * 6,
        out_specs=[VM] * 3,
        out_shape=FAR_OUT,
        scratch_shapes=[SLOTS_BY_FRAMES],
        compiler_params=PARAMS,
        name="numerators",
    )(place, column, proj, gram, got, far)


def mine_kernel(place, both, curv, mine):
    scatter(0, place[...], both[...], curv[:1, :], mine)


def scatter_mine(place, both, curv):
    return pl.pallas_call(
        mine_kernel,
        in_specs=[VM] * 3,
        out_specs=VM,
        out_shape=like(NBLK, ROWS, 128),
        compiler_params=PARAMS,
        cost_estimate=cost(512 * HALF * 256),
        name="scatter_mine",
    )(place, both, curv)


def fold_core_kernel(mine, came, *outs):
    for k in range(4):
        for q in range(4):
            outs[k][q] = mine[k * 4 + q] + came[k * 4 + q]


def fold_core(mine, came):
    return pl.pallas_call(
        fold_core_kernel,
        in_specs=[VM] * 2,
        out_specs=[VM] * 4,
        out_shape=[like(4, ROWS, 128)] * 4,
        compiler_params=PARAMS,
        name="fold_core",
    )(mine, came)


def fold_y_kernel(a, b, c, d, *outs):
    for k in range(4):
        outs[k][...] = (a[k] + b[k]) + (c[k] + d[k])


def fold_y(parts):
    return pl.pallas_call(
        fold_y_kernel,
        in_specs=[VM] * 4,
        out_specs=[VM] * 4,
        out_shape=[like(ROWS, 128)] * 4,
        compiler_params=PARAMS,
        name="fold_y",
    )(*parts)


def fold_z_kernel(a, b, c, d, out):
    out[...] = (a[...] + b[...]) + (c[...] + d[...])


def fold_z(parts):
    return pl.pallas_call(
        fold_z_kernel,
        in_specs=[VM] * 4,
        out_specs=VM,
        out_shape=like(ROWS, 128),
        compiler_params=PARAMS,
        name="fold_z",
    )(*parts)


def update_kernel(own, came, traces, out):
    a = as_column(own[64:65, :], 128)
    b = as_column(came[64:65, :], 128)
    for h in range(2):
        s = slice(h * 32, (h + 1) * 32)
        o = slice((1 - h) * 32, (2 - h) * 32)
        den = a[s] + b[o] + RIDGE
        out[s, :] = jnp.maximum(traces[s, :] + (own[s, :] + came[o, :]) / den, 0.0)


def update(own, came, traces):
    return pl.pallas_call(
        update_kernel,
        in_specs=[VM] * 3,
        out_specs=VM,
        out_shape=like(64, 128),
        compiler_params=PARAMS,
        name="update",
    )(own, came, traces)


def grad_kernel(column, got, far, foot, pairs, picked, out):
    picked[...] = got[...] + picked_from(1, column[...], far[...])
    out[512:, :] = jnp.zeros((8, 128), f32)

    def group(g, carry):
        s = rows_of(g)
        p = picked[s, :]
        gram = jnp.where(same_tile(), nt3(p, p), 0.0)
        out[pl.ds(512 + g, 1), :] = jnp.sum(gram, axis=0, keepdims=True)
        parts = []
        for t in range(GT):
            parts.append(correlate(p[t * SLOTS : (t + 1) * SLOTS], pairs[g * GT + t]))
        out[s, :] = jnp.concatenate(parts, axis=0) - nn3(gram, foot[s, :])
        return carry

    lax.fori_loop(0, NGROUP, group, 0)


def resident(pairs):
    return pltpu.with_memory_space_constraint(pairs, pltpu.VMEM)


def gradients(column, got, far, foot, pairs):
    return pl.pallas_call(
        grad_kernel,
        in_specs=[VM] * 5,
        out_specs=[VM] * 2,
        out_shape=[like(512, 128), like(520, 128)],
        compiler_params=PARAMS,
        name="gradients",
    )(column, got, far, foot, resident(pairs))


def stepped(g, parts, foot, valid):
    a, b, c, d = parts
    s = rows_of(g)
    row = pl.ds(512 + g, 1)
    dsp = (a[row, :] + c[row, :]) + (b[row, :] + d[row, :])
    total = (a[s, :] + c[s, :]) + (b[s, :] + d[s, :])
    return jnp.maximum(foot[s, :] + total / (as_column(dsp, 128) + RIDGE), 0.0) * valid[s, :]


def middle_kernel(
    place, a, b, c, d, foot, valid, picked, pairs, new, other, both, curv, work, sums
):
    def group(g, carry):
        s = rows_of(g)
        f = stepped(g, (a, b, c, d), foot, valid)
        new[s, :] = f
        gram = jnp.where(same_tile(), nt3(f, f), 0.0)
        sums[g] = jnp.broadcast_to(jnp.sum(gram, axis=0, keepdims=True), (8, 128))
        parts = []
        for t in range(GT):
            parts.append(project(f[t * SLOTS : (t + 1) * SLOTS], pairs[g * GT + t]))
        work[s, :] = jnp.concatenate(parts, axis=0) - nn3(gram, picked[s, :])
        return carry

    lax.fori_loop(0, NGROUP, group, 0)
    scatter_far(place, work, [sums[g, :1, :] for g in range(NGROUP)], other, both, curv)


def middle(place, parts, foot, valid, picked, pairs):
    return pl.pallas_call(
        middle_kernel,
        in_specs=[VM] * 9,
        out_specs=[VM] * 4,
        out_shape=[like(512, TILE)] + FAR_OUT,
        scratch_shapes=[SLOTS_BY_FRAMES, pltpu.VMEM((NGROUP, 8, 128), f32)],
        compiler_params=PARAMS,
        name="middle",
    )(place, *parts, foot, valid, picked, resident(pairs))


def last_kernel(a, b, c, d, foot, valid, new):
    for g in range(NGROUP):
        new[rows_of(g), :] = stepped(g, (a, b, c, d), foot, valid)


def last(parts, foot, valid):
    return pl.pallas_call(
        last_kernel,
        in_specs=[VM] * 6,
        out_specs=VM,
        out_shape=like(512, TILE),
        compiler_params=PARAMS,
        name="last",
    )(*parts, foot, valid)


def moved(x, axis, k):
    n = lax.axis_size(axis)
    return lax.ppermute(x, axis, [(i, (i + k) % n) for i in range(n)])


def swapped(x, axis, bits):
    n = lax.axis_size(axis)
    return lax.ppermute(x, axis, [(i, i ^ bits) for i in range(n)])


def across(x):
    return swapped(x, ("zh", "zl"), 7)


def summed_blocks(place, other, both, curv):
    came = swapped(other, "c", 1)
    ys = fold_core(scatter_mine(place, both, curv), came)
    far = [moved(ys[k], "y", k) for k in (2, 1, 3)]
    zs = fold_y([ys[0]] + far)
    far = [swapped(zs[k], "zl", k) for k in (3, 2, 1)]
    own = fold_z([zs[0]] + far)
    return own, across(own)


def along_z(block):
    c, b, a = (swapped(block, "zl", k) for k in (3, 2, 1))
    return jnp.concatenate([block, a, b, c], axis=0)


def along_y(mine):
    b, a, c = (moved(mine, "y", -k) for k in (2, 1, 3))
    return jnp.concatenate([mine, a, b, c], axis=0)


def over_frames(x):
    two, one, three = (moved(x, "ta", k) for k in (2, 1, 3))
    return x, one, two, three


def local(movie, traces, entry_comp, footprints):
    zh, y, c, zl = (lax.axis_index(name) for name in BLOCKS)
    owner = entry_comp // 32
    ozh, oy, oc, ozl = owner // 32, (owner // 8) % 4, (owner // 4) % 2, owner % 4
    block = ((oc ^ c) * 4 + (oy - y) % 4) * 4 + (ozl ^ (3 * ozh) ^ zl ^ (3 * zh))
    index = (block * 64 + (ozh ^ zh) * 32 + entry_comp % 32).reshape(-1)
    place = jnp.where(entry_comp.reshape(-1) < K, index, K)[None, :]
    column, valid, foot = prepare(place, footprints.reshape(-1, TILE))

    own = jnp.concatenate([traces, across(traces)], axis=0)
    mine = along_z(own)
    mine, foot, place, column, valid = lax.optimization_barrier(
        (mine, foot, place, column, valid)
    )
    near = along_y(mine)
    near, pairs, proj, gram = lax.optimization_barrier((near, *first(movie, foot)))
    far = swapped(near, "c", 1)
    sums = numerators(place, column, proj, gram, pick_near(column, near), far)
    for step in range(ITERS):
        own = update(*summed_blocks(place, *sums), own)
        near = along_y(along_z(own))
        far = swapped(near, "c", 1)
        picked, grad = gradients(column, pick_near(column, near), far, foot, pairs)
        parts = over_frames(grad)
        if step + 1 < ITERS:
            foot, *sums = middle(place, parts, foot, valid, picked, pairs)
        else:
            foot = last(parts, foot, valid)
    return own[:32], foot.reshape(footprints.shape)


def solution(mesh):
    torus = Mesh(
        mesh.devices.reshape(2, 4, 2, mesh.shape["gy"], mesh.shape["ta"]),
        ("zh", "y", "c", "zl", "ta"),
    )
    in_specs = (P(BLOCKS, "ta"), P(BLOCKS, "ta"), P(BLOCKS, None), P(BLOCKS, None, None))
    out_specs = (P(BLOCKS, "ta"), P(BLOCKS, None, None))
    return jax.shard_map(local, mesh=torus, in_specs=in_specs, out_specs=out_specs, check_vma=False)
```

```python
import functools

import jax
import jax.numpy as jnp
from jax import lax
from jax.experimental import pallas as pl
from jax.experimental.pallas import tpu as pltpu
from jax.sharding import Mesh
from jax.sharding import PartitionSpec as P


K = 2048
TILE = 128
SLOTS = 8
ITERS = 2
RIDGE = 1.0
BLOCKS = ("zh", "y", "c", "zl")
NGROUP = 4
GT = 16
UNROLL = 8
HALF = 1024
NBLK = 16
ROWS = 72
WIDE = 264

VM = pl.BlockSpec(memory_space=pltpu.VMEM)
HB = pl.BlockSpec(memory_space=pltpu.HBM)
PARAMS = pltpu.CompilerParams(vmem_limit_bytes=24 * 1024 * 1024)
f32 = jnp.float32
bf16 = jnp.bfloat16


def like(*shape, dtype=f32):
    return jax.ShapeDtypeStruct(shape, dtype)


def cost(macs):
    return pl.CostEstimate(flops=2 * macs, bytes_accessed=1 << 20, transcendentals=0)


def split(x):
    hi = x.astype(bf16)
    lo = (x - hi.astype(f32)).astype(bf16)
    return hi, lo


def nt(a, b):
    return lax.dot_general(a, b, (((1,), (1,)), ((), ())), preferred_element_type=f32)


def nn(a, b):
    return lax.dot_general(a, b, (((1,), (0,)), ((), ())), preferred_element_type=f32)


def nt3(a, b):
    ah, al = split(a)
    bh, bl = split(b)
    return nt(ah, bh) + (nt(ah, bl) + nt(al, bh))


def nn3(a, b):
    ah, al = split(a)
    bh, bl = split(b)
    return nn(ah, bh) + (nn(ah, bl) + nn(al, bh))


def same_tile():
    i = lax.broadcasted_iota(jnp.int32, (128, 128), 0) // SLOTS
    j = lax.broadcasted_iota(jnp.int32, (128, 128), 1) // SLOTS
    return i == j


def stacked(x):
    hi = x.astype(bf16).astype(f32)
    return jnp.concatenate([hi, x - hi], axis=0).astype(bf16)


def as_column(row, n):
    i = lax.broadcasted_iota(jnp.int32, (n, n), 0)
    j = lax.broadcasted_iota(jnp.int32, (n, n), 1)
    return jnp.sum(jnp.where(i == j, row, 0.0), axis=1, keepdims=True)


def project(foot, pair):
    two = stacked(foot)
    out = nn(jnp.concatenate([two, two], axis=1), pair)
    return out[:SLOTS] + out[SLOTS:]


def correlate(picked, pair):
    out = nt(stacked(picked), pair)
    out = out[:SLOTS] + out[SLOTS:]
    return out[:, :TILE] + out[:, TILE:]


def rows_of(g):
    return pl.ds(pl.multiple_of(g * 128, 128), 128)


def first_kernel(
    entry, movie, footprints, place, column, valid, foot, pairs, proj, gram, frames, came, got
):
    zh, y, c, zl = (lax.axis_index(name) for name in BLOCKS)
    x = lax.axis_index("ta")
    tall = GT * TILE
    for k in range(NGROUP):
        g = x ^ k
        at = pl.ds(pl.multiple_of(g * 128, 128), 128)
        pltpu.make_async_copy(footprints.at[at], foot.at[pl.ds(k * 128, 128)], got.at[k]).start()
        at = pl.ds(pl.multiple_of(g * tall, tall), tall)
        pltpu.make_async_copy(movie.at[at], frames.at[pl.ds(k * tall, tall)], came.at[k]).start()
    for k in range(NGROUP):
        s = slice(k * 128, (k + 1) * 128)
        comp = entry[x ^ k]
        owner = comp >> 5
        ozh, oy, oc, ozl = owner >> 5, (owner >> 3) & 3, (owner >> 2) & 1, owner & 3
        block = ((oc ^ c) * 4 + (oy ^ y)) * 4 + (ozl ^ (3 * ozh) ^ zl ^ (3 * zh))
        index = jnp.where(comp < K, block * 64 + (ozh ^ zh) * 32 + (comp & 31), K)
        place[:, s] = index
        at = as_column(index.astype(f32), 128)
        column[s, :] = at.astype(jnp.int32)
        valid[s, :] = jnp.where(at < K, 1.0, 0.0)

    def group(k, carry):
        s = rows_of(k)
        pltpu.make_async_copy(footprints.at[s], foot.at[s], got.at[k]).wait()
        f = foot[s, :] * valid[s, :]
        foot[s, :] = f
        gram[k] = jnp.where(same_tile(), nt3(f, f), 0.0)
        at = pl.ds(pl.multiple_of(k * tall, tall), tall)
        pltpu.make_async_copy(movie.at[at], frames.at[at], came.at[k]).wait()
        parts = []
        for t in range(GT):
            at = pl.ds(pl.multiple_of((k * GT + t) * TILE, TILE), TILE)
            hi, lo = split(frames[at, :])
            pair = jnp.concatenate([hi, lo], axis=0)
            pairs[k * GT + t] = pair
            parts.append(project(f[t * SLOTS : (t + 1) * SLOTS], pair))
        proj[s, :] = jnp.concatenate(parts, axis=0)
        return carry

    lax.fori_loop(0, NGROUP, group, 0)


def first(entry, movie, footprints):
    return pl.pallas_call(
        first_kernel,
        in_specs=[VM, HB, HB],
        out_specs=[VM] * 7,
        out_shape=[
            like(1, 512, dtype=jnp.int32),
            like(512, 1, dtype=jnp.int32),
            like(512, 1),
            like(512, TILE),
            pltpu.VMEM((64, 2 * TILE, 128), bf16),
            like(512, 128),
            like(NGROUP, 128, 128),
        ],
        scratch_shapes=[
            pltpu.VMEM((64 * TILE, 128), f32),
            pltpu.SemaphoreType.DMA((NGROUP,)),
            pltpu.SemaphoreType.DMA((NGROUP,)),
        ],
        compiler_params=PARAMS,
        cost_estimate=cost(64 * 16 * 256 * 128),
        name="first",
    )(
        entry,
        pltpu.with_memory_space_constraint(movie, pltpu.HBM),
        pltpu.with_memory_space_constraint(footprints, pltpu.HBM),
    )


def scatter(half, place, both, curv, out):
    n = place.shape[1]
    lane = lax.broadcasted_iota(jnp.int32, (256, n), 0)
    inside = jnp.where(lane[:128] == place % 64, 1.0, 0.0).astype(bf16)
    block = lax.broadcasted_iota(jnp.int32, (NBLK, n), 0) + half * NBLK
    ch, cl = split(jnp.where(block == place // 64, curv, 0.0))
    den = nt(ch, inside) + nt(cl, inside)
    dens = jnp.concatenate([den, jnp.zeros((8, 128), f32)], axis=0)
    for k in range(4):
        out[k, 256:, :] = dens[k * 4 : k * 4 + 8]

    def block_rows(k, carry):
        hot = jnp.where(lane + (half * HALF + k * 256) == place, 1.0, 0.0).astype(bf16)
        got = nn(hot, both)
        out[k, :256, :] = got[:, :128] + got[:, 128:]
        return carry

    lax.fori_loop(0, 4, block_rows, 0)


def picked_from(half, column, part, add, out):
    both = jnp.concatenate(split(part[...]), axis=1)
    lane = lax.broadcasted_iota(jnp.int32, (256, HALF), 1) + half * HALF

    def some(i, carry):
        s = pl.ds(pl.multiple_of(i * 256, 256), 256)
        hot = jnp.where(lane == column[s, :], 1.0, 0.0).astype(bf16)
        got = nn(hot, both)
        got = got[:, :128] + got[:, 128:]
        out[s, :] = got if add is None else got + add[s, :]
        return carry

    lax.fori_loop(0, 2, some, 0)


def near_kernel(column, near, out):
    picked_from(0, column, near, None, out)


def pick_near(column, near):
    return pl.pallas_call(
        near_kernel,
        in_specs=[VM] * 2,
        out_specs=VM,
        out_shape=like(512, 128),
        compiler_params=PARAMS,
        cost_estimate=cost(512 * HALF * 256),
        name="pick_near",
    )(column, near)


SLOTS_BY_FRAMES = pltpu.VMEM((512, 128), f32)
FAR_OUT = [like(4, WIDE, 128), like(512, 256, dtype=bf16), like(8, 512)]


def scatter_far(place, work, rows, other, both, curv):
    two = jnp.concatenate(split(work[...]), axis=1)
    row = jnp.concatenate(rows, axis=1)
    both[...] = two
    curv[...] = jnp.broadcast_to(row, (8, 512))
    scatter(1, place[...], two, row, other)


def numer_kernel(place, column, proj, gram, got, far, other, both, curv, work):
    picked_from(1, column, far, got, work)
    rows = []
    for g in range(NGROUP):
        s = slice(g * 128, (g + 1) * 128)
        work[s, :] = proj[s, :] - nn3(gram[g], work[s, :])
        rows.append(jnp.sum(gram[g], axis=0, keepdims=True))
    scatter_far(place, work, rows, other, both, curv)


def numerators(place, column, proj, gram, got, far):
    return pl.pallas_call(
        numer_kernel,
        in_specs=[VM] * 6,
        out_specs=[VM] * 3,
        out_shape=FAR_OUT,
        scratch_shapes=[SLOTS_BY_FRAMES],
        compiler_params=PARAMS,
        name="numerators",
    )(place, column, proj, gram, got, far)


def mine_kernel(place, both, curv, mine):
    scatter(0, place[...], both[...], curv[:1, :], mine)


def scatter_mine(place, both, curv):
    return pl.pallas_call(
        mine_kernel,
        in_specs=[VM] * 3,
        out_specs=VM,
        out_shape=like(4, WIDE, 128),
        compiler_params=PARAMS,
        cost_estimate=cost(512 * HALF * 256),
        name="scatter_mine",
    )(place, both, curv)


def fold_core_kernel(mine, came, *outs):
    for k in range(4):
        outs[k][...] = mine[k] + came[k]


def fold_core(mine, came):
    return pl.pallas_call(
        fold_core_kernel,
        in_specs=[VM] * 2,
        out_specs=[VM] * 4,
        out_shape=[like(WIDE, 128)] * 4,
        compiler_params=PARAMS,
        name="fold_core",
    )(mine, came)


def fold_y_kernel(a, b, c, d, *outs):
    den = (a[256:, :] + b[256:, :]) + (c[256:, :] + d[256:, :])
    for k in range(4):
        s = slice(k * 64, (k + 1) * 64)
        outs[k][:64, :] = (a[s, :] + b[s, :]) + (c[s, :] + d[s, :])
        outs[k][64:, :] = jnp.broadcast_to(den[k : k + 1], (8, 128))


def fold_y(parts):
    return pl.pallas_call(
        fold_y_kernel,
        in_specs=[VM] * 4,
        out_specs=[VM] * 4,
        out_shape=[like(ROWS, 128)] * 4,
        compiler_params=PARAMS,
        name="fold_y",
    )(*parts)


def fold_z_kernel(a, b, c, d, out):
    out[...] = (a[...] + b[...]) + (c[...] + d[...])


def fold_z(parts):
    return pl.pallas_call(
        fold_z_kernel,
        in_specs=[VM] * 4,
        out_specs=VM,
        out_shape=like(ROWS, 128),
        compiler_params=PARAMS,
        name="fold_z",
    )(*parts)


def update_kernel(own, came, traces, out):
    a = as_column(own[64:65, :], 128)
    b = as_column(came[64:65, :], 128)
    for h in range(2):
        s = slice(h * 32, (h + 1) * 32)
        o = slice((1 - h) * 32, (2 - h) * 32)
        den = a[s] + b[o] + RIDGE
        out[s, :] = jnp.maximum(traces[s, :] + (own[s, :] + came[o, :]) / den, 0.0)


def update(own, came, traces):
    return pl.pallas_call(
        update_kernel,
        in_specs=[VM] * 3,
        out_specs=VM,
        out_shape=like(64, 128),
        compiler_params=PARAMS,
        name="update",
    )(own, came, traces)


def resident(pairs):
    return pltpu.with_memory_space_constraint(pairs, pltpu.VMEM)


def grad_piece(k, picked, foot, pairs, out):
    p = picked[k * 128 : (k + 1) * 128, :]
    gram = jnp.where(same_tile(), nt3(p, p), 0.0)
    out[128:, :] = jnp.broadcast_to(jnp.sum(gram, axis=0, keepdims=True), (8, 128))
    out[:128, :] = -nn3(gram, foot[k * 128 : (k + 1) * 128, :])

    def tiles(i, carry):
        for j in range(UNROLL):
            t = i * UNROLL + j
            at = pl.ds(pl.multiple_of(k * 128 + t * SLOTS, SLOTS), SLOTS)
            rows = pl.ds(pl.multiple_of(t * SLOTS, SLOTS), SLOTS)
            out[rows, :] += correlate(picked[at, :], pairs[k * GT + t])
        return carry

    lax.fori_loop(0, GT // UNROLL, tiles, 0)


def picked_grad_kernel(k, column, got, far, foot, pairs, picked, out):
    picked_from(1, column, far, got, picked)
    grad_piece(k, picked, foot, pairs, out)


def picked_gradient(k, column, got, far, foot, pairs):
    return pl.pallas_call(
        functools.partial(picked_grad_kernel, k),
        in_specs=[VM] * 5,
        out_specs=[VM] * 2,
        out_shape=[like(512, 128), like(136, 128)],
        compiler_params=PARAMS,
        cost_estimate=cost(512 * HALF * 256),
        name="picked_gradient",
    )(column, got, far, foot, resident(pairs))


def grad_kernel(k, picked, foot, pairs, out):
    grad_piece(k, picked, foot, pairs, out)


def gradient(k, picked, foot, pairs):
    return pl.pallas_call(
        functools.partial(grad_kernel, k),
        in_specs=[VM] * 3,
        out_specs=VM,
        out_shape=like(136, 128),
        compiler_params=PARAMS,
        cost_estimate=cost(16 * 16 * 256 * 128),
        name="gradient",
    )(picked, foot, resident(pairs))


def step_kernel(a, b, c, d, foot, valid, new):
    total = (a[...] + c[...]) + (b[...] + d[...])
    dsp = as_column(total[128:129, :], 128) + RIDGE
    new[...] = jnp.maximum(foot[:128, :] + total[:128] / dsp, 0.0) * valid[:128, :]


def stepped(parts, foot, valid):
    return pl.pallas_call(
        step_kernel,
        in_specs=[VM] * 6,
        out_specs=VM,
        out_shape=like(128, TILE),
        compiler_params=PARAMS,
        name="step",
    )(*parts, foot, valid)


def again_kernel(k, foot, picked, pairs, work, curv):
    f = foot[...]
    gram = jnp.where(same_tile(), nt3(f, f), 0.0)
    curv[...] = jnp.broadcast_to(jnp.sum(gram, axis=0, keepdims=True), (8, 128))
    work[...] = -nn3(gram, picked[k * 128 : (k + 1) * 128, :])

    def tiles(i, carry):
        for j in range(UNROLL):
            t = i * UNROLL + j
            rows = pl.ds(pl.multiple_of(t * SLOTS, SLOTS), SLOTS)
            work[rows, :] += project(foot[rows, :], pairs[k * GT + t])
        return carry

    lax.fori_loop(0, GT // UNROLL, tiles, 0)


def projected(k, foot, picked, pairs):
    return pl.pallas_call(
        functools.partial(again_kernel, k),
        in_specs=[VM] * 3,
        out_specs=[VM] * 2,
        out_shape=[like(128, 128), like(8, 128)],
        compiler_params=PARAMS,
        cost_estimate=cost(16 * 16 * 256 * 128),
        name="projected",
    )(foot, picked, resident(pairs))


def far_kernel(place, w0, w1, w2, w3, c0, c1, c2, c3, other, both, curv, work):
    for k, part in enumerate((w0, w1, w2, w3)):
        work[k * 128 : (k + 1) * 128, :] = part[...]
    scatter_far(place, work, [c[:1, :] for c in (c0, c1, c2, c3)], other, both, curv)


def scatter_other(place, works, curvs):
    return pl.pallas_call(
        far_kernel,
        in_specs=[VM] * 9,
        out_specs=[VM] * 3,
        out_shape=FAR_OUT,
        scratch_shapes=[SLOTS_BY_FRAMES],
        compiler_params=PARAMS,
        name="scatter_other",
    )(place, *works, *curvs)


def last_kernel(f0, f1, f2, f3, new):
    x = lax.axis_index("ta")
    for k, foot in enumerate((f0, f1, f2, f3)):
        new[rows_of(x ^ k), :] = foot[...]


def last(feet):
    return pl.pallas_call(
        last_kernel,
        in_specs=[VM] * 4,
        out_specs=VM,
        out_shape=like(512, TILE),
        compiler_params=PARAMS,
        name="last",
    )(*feet)


def swapped(x, axis, bits):
    n = lax.axis_size(axis)
    return lax.ppermute(x, axis, [(i, i ^ bits) for i in range(n)])


def across(x):
    return swapped(x, ("zh", "zl"), 7)


def summed_blocks(place, other, both, curv):
    came = swapped(other, "c", 1)
    ys = fold_core(scatter_mine(place, both, curv), came)
    zs = fold_y([ys[0]] + [swapped(ys[k], "y", k) for k in (2, 1, 3)])
    own = fold_z([zs[0]] + [swapped(zs[k], "zl", k) for k in (3, 2, 1)])
    return own, across(own)


def gathered(part, axis):
    near = [swapped(part, axis, k) for k in (1, 2, 3)]
    return jnp.concatenate([part] + near, axis=0)


def new_feet(column, near, far, foot, valid, pairs):
    picked, piece = picked_gradient(2, column, pick_near(column, near), far, foot, pairs)
    came = {2: swapped(piece, "ta", 2)}
    for k in (1, 3):
        piece = gradient(k, picked, foot, pairs)
        came[k] = swapped(piece, "ta", k)
    came[0] = gradient(0, picked, foot, pairs)
    own = stepped([came[k] for k in range(NGROUP)], foot, valid)
    return [own] + [swapped(own, "ta", k) for k in (1, 2, 3)], picked


def local(movie, traces, entry_comp, footprints):
    own = jnp.concatenate([traces, across(traces)], axis=0)
    entry = entry_comp.reshape(NGROUP, 1, 128)
    near = gathered(gathered(own, "zl"), "y")
    made = first(entry, movie, footprints.reshape(-1, TILE))
    near, place, column, valid, foot, pairs, proj, gram = lax.optimization_barrier((near, *made))
    far = swapped(near, "c", 1)
    sums = numerators(place, column, proj, gram, pick_near(column, near), far)
    for step in range(ITERS):
        own = update(*summed_blocks(place, *sums), own)
        near = gathered(gathered(own, "zl"), "y")
        far = swapped(near, "c", 1)
        feet, picked = new_feet(column, near, far, foot, valid, pairs)
        if step + 1 < ITERS:
            works, curvs = zip(*(projected(k, feet[k], picked, pairs) for k in range(NGROUP)))
            sums = scatter_other(place, works, curvs)
            foot = jnp.concatenate(feet, axis=0)
    return own[:32], last(feet).reshape(footprints.shape)


def solution(mesh):
    torus = Mesh(
        mesh.devices.reshape(2, 4, 2, mesh.shape["gy"], mesh.shape["ta"]),
        ("zh", "y", "c", "zl", "ta"),
    )
    in_specs = (P(BLOCKS, "ta"), P(BLOCKS, "ta"), P(BLOCKS, None), P(BLOCKS, None, None))
    out_specs = (P(BLOCKS, "ta"), P(BLOCKS, None, None))
    return jax.shard_map(local, mesh=torus, in_specs=in_specs, out_specs=out_specs, check_vma=False)
```

```python
import functools

import jax
import jax.numpy as jnp
from jax import lax
from jax.experimental import pallas as pl
from jax.experimental.pallas import tpu as pltpu
from jax.sharding import Mesh
from jax.sharding import PartitionSpec as P


K = 2048
TILE = 128
SLOTS = 8
ITERS = 2
RIDGE = 1.0
BLOCKS = ("zh", "y", "c", "zl")
NGROUP = 4
GT = 16
HALF = 1024
NBLK = 16
ROWS = 72
WIDE = 264

VM = pl.BlockSpec(memory_space=pltpu.VMEM)
HB = pl.BlockSpec(memory_space=pltpu.HBM)
PARAMS = pltpu.CompilerParams(vmem_limit_bytes=24 * 1024 * 1024)
f32 = jnp.float32
bf16 = jnp.bfloat16


def like(*shape, dtype=f32):
    return jax.ShapeDtypeStruct(shape, dtype)


def cost(macs):
    return pl.CostEstimate(flops=2 * macs, bytes_accessed=1 << 20, transcendentals=0)


def split(x):
    hi = x.astype(bf16)
    lo = (x - hi.astype(f32)).astype(bf16)
    return hi, lo


def nt(a, b):
    return lax.dot_general(a, b, (((1,), (1,)), ((), ())), preferred_element_type=f32)


def nn(a, b):
    return lax.dot_general(a, b, (((1,), (0,)), ((), ())), preferred_element_type=f32)


def nt3(a, b):
    ah, al = split(a)
    bh, bl = split(b)
    return nt(ah, bh) + (nt(ah, bl) + nt(al, bh))


def nn3(a, b):
    ah, al = split(a)
    bh, bl = split(b)
    return nn(ah, bh) + (nn(ah, bl) + nn(al, bh))


def same_tile():
    i = lax.broadcasted_iota(jnp.int32, (128, 128), 0) // SLOTS
    j = lax.broadcasted_iota(jnp.int32, (128, 128), 1) // SLOTS
    return i == j


def stacked(x):
    hi = x.astype(bf16).astype(f32)
    return jnp.concatenate([hi, x - hi], axis=0).astype(bf16)


def as_column(row, n):
    i = lax.broadcasted_iota(jnp.int32, (n, n), 0)
    j = lax.broadcasted_iota(jnp.int32, (n, n), 1)
    return jnp.sum(jnp.where(i == j, row, 0.0), axis=1, keepdims=True)


def project(foot, pair):
    two = stacked(foot)
    out = nn(jnp.concatenate([two, two], axis=1), pair)
    return out[:SLOTS] + out[SLOTS:]


def correlate(picked, pair):
    out = nt(stacked(picked), pair)
    out = out[:SLOTS] + out[SLOTS:]
    return out[:, :TILE] + out[:, TILE:]


def rows_of(g):
    return pl.ds(pl.multiple_of(g * 128, 128), 128)


def first_kernel(
    entry, movie, footprints, place, column, valid, foot, pairs, proj, gram, frames, came, got
):
    zh, y, c, zl = (lax.axis_index(name) for name in BLOCKS)
    x = lax.axis_index("ta")
    tall = GT * TILE
    for k in range(NGROUP):
        g = x ^ k
        at = pl.ds(pl.multiple_of(g * 128, 128), 128)
        pltpu.make_async_copy(footprints.at[at], foot.at[pl.ds(k * 128, 128)], got.at[k]).start()
        at = pl.ds(pl.multiple_of(g * tall, tall), tall)
        pltpu.make_async_copy(movie.at[at], frames.at[pl.ds(k * tall, tall)], came.at[k]).start()
    for k in range(NGROUP):
        s = slice(k * 128, (k + 1) * 128)
        comp = entry[x ^ k]
        owner = comp >> 5
        ozh, oy, oc, ozl = owner >> 5, (owner >> 3) & 3, (owner >> 2) & 1, owner & 3
        row = ((oc ^ c) * 4 + (oy ^ y)) * 256 + (comp & 31)
        index = row + (ozl ^ (3 * ozh) ^ zl ^ (3 * zh)) * 64 + (ozh ^ zh) * 32
        index = jnp.where(comp < K, index, K)
        place[:, s] = index
        at = as_column(index.astype(f32), 128)
        column[s, :] = at.astype(jnp.int32)
        valid[s, :] = jnp.where(at < K, 1.0, 0.0)

    def group(k, carry):
        s = rows_of(k)
        pltpu.make_async_copy(footprints.at[s], foot.at[s], got.at[k]).wait()
        f = foot[s, :] * valid[s, :]
        foot[s, :] = f
        gram[k] = jnp.where(same_tile(), nt3(f, f), 0.0)
        at = pl.ds(pl.multiple_of(k * tall, tall), tall)
        pltpu.make_async_copy(movie.at[at], frames.at[at], came.at[k]).wait()
        parts = []
        for t in range(GT):
            at = pl.ds(pl.multiple_of((k * GT + t) * TILE, TILE), TILE)
            hi, lo = split(frames[at, :])
            pair = jnp.concatenate([hi, lo], axis=0)
            pairs[k * GT + t] = pair
            parts.append(project(f[t * SLOTS : (t + 1) * SLOTS], pair))
        proj[s, :] = jnp.concatenate(parts, axis=0)
        return carry

    lax.fori_loop(0, NGROUP, group, 0)


def first(entry, movie, footprints):
    return pl.pallas_call(
        first_kernel,
        in_specs=[VM, HB, HB],
        out_specs=[VM] * 7,
        out_shape=[
            like(1, 512, dtype=jnp.int32),
            like(512, 1, dtype=jnp.int32),
            like(512, 1),
            like(512, TILE),
            pltpu.VMEM((64, 2 * TILE, 128), bf16),
            like(512, 128),
            like(NGROUP, 128, 128),
        ],
        scratch_shapes=[
            pltpu.VMEM((64 * TILE, 128), f32),
            pltpu.SemaphoreType.DMA((NGROUP,)),
            pltpu.SemaphoreType.DMA((NGROUP,)),
        ],
        compiler_params=PARAMS,
        cost_estimate=cost(64 * 16 * 256 * 128),
        name="first",
    )(
        entry,
        pltpu.with_memory_space_constraint(movie, pltpu.HBM),
        pltpu.with_memory_space_constraint(footprints, pltpu.HBM),
    )


def scatter(half, place, both, curv, out, looped):
    n = place.shape[1]
    lane = lax.broadcasted_iota(jnp.int32, (256, n), 0)
    inside = jnp.where(lane[:128] == place % 64, 1.0, 0.0).astype(bf16)
    block = lax.broadcasted_iota(jnp.int32, (NBLK, n), 0) + half * NBLK
    ch, cl = split(jnp.where(block == place // 64, curv, 0.0))
    den = nt(ch, inside) + nt(cl, inside)
    dens = jnp.concatenate([den, jnp.zeros((8, 128), f32)], axis=0)
    for k in range(4):
        out[k, 256:, :] = dens[k * 4 : k * 4 + 8]

    def rows(k, carry):
        hot = jnp.where(lane + (half * HALF + k * 256) == place, 1.0, 0.0).astype(bf16)
        got = nn(hot, both[...])
        out[k, :256, :] = got[:, :128] + got[:, 128:]
        return carry

    if looped:
        lax.fori_loop(0, 4, rows, 0)
    else:
        for k in range(4):
            rows(k, 0)


def picked_from_far(column, far, near, out):
    both = jnp.concatenate(split(far[...]), axis=1)
    at = column[...]
    lane = lax.broadcasted_iota(jnp.int32, (at.shape[0], HALF), 1) + HALF
    got = nn(jnp.where(lane == at, 1.0, 0.0).astype(bf16), both)
    out[...] = got[:, :128] + got[:, 128:] + near[...]


def near_kernel(column, near, out):
    both = jnp.concatenate(split(near[...]), axis=1)
    lane = lax.broadcasted_iota(jnp.int32, (256, HALF), 1)

    def some(i, carry):
        s = pl.ds(pl.multiple_of(i * 256, 256), 256)
        hot = jnp.where(lane == column[s, :], 1.0, 0.0).astype(bf16)
        got = nn(hot, both)
        out[s, :] = got[:, :128] + got[:, 128:]
        return carry

    lax.fori_loop(0, 2, some, 0)


def pick_near(column, near):
    return pl.pallas_call(
        near_kernel,
        in_specs=[VM] * 2,
        out_specs=VM,
        out_shape=like(512, 128),
        compiler_params=PARAMS,
        cost_estimate=cost(512 * HALF * 256),
        name="pick_near",
    )(column, near)


SLOTS_BY_FRAMES = pltpu.VMEM((512, 128), f32)
FAR_OUT = [like(4, WIDE, 128), like(512, 256, dtype=bf16), like(8, 512)]


def scatter_far(place, work, rows, other, both, curv):
    two = jnp.concatenate(split(work[...]), axis=1)
    row = jnp.concatenate(rows, axis=1)
    both[...] = two
    curv[...] = jnp.broadcast_to(row, (8, 512))
    scatter(1, place[...], two, row, other, False)


def numer_kernel(place, column, proj, gram, got, far, other, both, curv, work):
    picked_from_far(column, far, got, work)
    rows = []
    for g in range(NGROUP):
        s = slice(g * 128, (g + 1) * 128)
        work[s, :] = proj[s, :] - nn3(gram[g], work[s, :])
        rows.append(jnp.sum(gram[g], axis=0, keepdims=True))
    scatter_far(place, work, rows, other, both, curv)


def numerators(place, column, proj, gram, got, far):
    return pl.pallas_call(
        numer_kernel,
        in_specs=[VM] * 6,
        out_specs=[VM] * 3,
        out_shape=FAR_OUT,
        scratch_shapes=[SLOTS_BY_FRAMES],
        compiler_params=PARAMS,
        name="numerators",
    )(place, column, proj, gram, got, far)


def mine_kernel(place, both, curv, mine):
    scatter(0, place[...], both, curv[:1, :], mine, True)


def scatter_mine(place, both, curv):
    return pl.pallas_call(
        mine_kernel,
        in_specs=[VM] * 3,
        out_specs=VM,
        out_shape=like(4, WIDE, 128),
        compiler_params=PARAMS,
        cost_estimate=cost(512 * HALF * 256),
        name="scatter_mine",
    )(place, both, curv)


def fold_core_kernel(mine, came, *outs):
    for k in range(4):
        outs[k][...] = mine[k] + came[k]


def fold_core(mine, came):
    return pl.pallas_call(
        fold_core_kernel,
        in_specs=[VM] * 2,
        out_specs=[VM] * 4,
        out_shape=[like(WIDE, 128)] * 4,
        compiler_params=PARAMS,
        name="fold_core",
    )(mine, came)


def fold_y_kernel(a, b, c, d, *outs):
    den = (a[256:, :] + b[256:, :]) + (c[256:, :] + d[256:, :])
    for k in range(4):
        s = slice(k * 64, (k + 1) * 64)
        outs[k][:64, :] = (a[s, :] + b[s, :]) + (c[s, :] + d[s, :])
        outs[k][64:, :] = jnp.broadcast_to(den[k : k + 1], (8, 128))


def fold_y(parts):
    return pl.pallas_call(
        fold_y_kernel,
        in_specs=[VM] * 4,
        out_specs=[VM] * 4,
        out_shape=[like(ROWS, 128)] * 4,
        compiler_params=PARAMS,
        name="fold_y",
    )(*parts)


def fold_z_kernel(a, b, c, d, out):
    out[...] = (a[...] + b[...]) + (c[...] + d[...])


def fold_z(parts):
    return pl.pallas_call(
        fold_z_kernel,
        in_specs=[VM] * 4,
        out_specs=VM,
        out_shape=like(ROWS, 128),
        compiler_params=PARAMS,
        name="fold_z",
    )(*parts)


def update_kernel(own, came, traces, out):
    a = as_column(own[64:65, :], 128)
    b = as_column(came[64:65, :], 128)
    for h in range(2):
        s = slice(h * 32, (h + 1) * 32)
        o = slice((1 - h) * 32, (2 - h) * 32)
        den = a[s] + b[o] + RIDGE
        out[s, :] = jnp.maximum(traces[s, :] + (own[s, :] + came[o, :]) / den, 0.0)


def update(own, came, traces):
    return pl.pallas_call(
        update_kernel,
        in_specs=[VM] * 3,
        out_specs=VM,
        out_shape=like(64, 128),
        compiler_params=PARAMS,
        name="update",
    )(own, came, traces)


def resident(pairs):
    return pltpu.with_memory_space_constraint(pairs, pltpu.VMEM)


def grad_piece(k, picked, foot, pairs, out):
    p = picked[k * 128 : (k + 1) * 128, :]
    gram = jnp.where(same_tile(), nt3(p, p), 0.0)
    out[128:, :] = jnp.broadcast_to(jnp.sum(gram, axis=0, keepdims=True), (8, 128))
    parts = []
    for t in range(GT):
        parts.append(correlate(p[t * SLOTS : (t + 1) * SLOTS], pairs[k * GT + t]))
    less = nn3(gram, foot[k * 128 : (k + 1) * 128, :])
    out[:128, :] = jnp.concatenate(parts, axis=0) - less


def picked_grad_kernel(k, column, got, far, foot, pairs, picked, out):
    picked_from_far(column, far, got, picked)
    grad_piece(k, picked, foot, pairs, out)


def picked_gradient(k, column, got, far, foot, pairs):
    return pl.pallas_call(
        functools.partial(picked_grad_kernel, k),
        in_specs=[VM] * 5,
        out_specs=[VM] * 2,
        out_shape=[like(512, 128), like(136, 128)],
        compiler_params=PARAMS,
        cost_estimate=cost(512 * HALF * 256),
        name="picked_gradient",
    )(column, got, far, foot, resident(pairs))


def grad_kernel(k, picked, foot, pairs, out):
    grad_piece(k, picked, foot, pairs, out)


def gradient(k, picked, foot, pairs):
    return pl.pallas_call(
        functools.partial(grad_kernel, k),
        in_specs=[VM] * 3,
        out_specs=VM,
        out_shape=like(136, 128),
        compiler_params=PARAMS,
        cost_estimate=cost(16 * 16 * 256 * 128),
        name="gradient",
    )(picked, foot, resident(pairs))


def step_kernel(a, b, c, d, foot, valid, new):
    total = (a[...] + c[...]) + (b[...] + d[...])
    dsp = as_column(total[128:129, :], 128) + RIDGE
    new[...] = jnp.maximum(foot[:128, :] + total[:128] / dsp, 0.0) * valid[:128, :]


def stepped(parts, foot, valid):
    return pl.pallas_call(
        step_kernel,
        in_specs=[VM] * 6,
        out_specs=VM,
        out_shape=like(128, TILE),
        compiler_params=PARAMS,
        name="step",
    )(*parts, foot, valid)


def again_kernel(k, foot, picked, pairs, work, curv):
    f = foot[...]
    gram = jnp.where(same_tile(), nt3(f, f), 0.0)
    curv[...] = jnp.broadcast_to(jnp.sum(gram, axis=0, keepdims=True), (8, 128))
    parts = []
    for t in range(GT):
        parts.append(project(f[t * SLOTS : (t + 1) * SLOTS], pairs[k * GT + t]))
    less = nn3(gram, picked[k * 128 : (k + 1) * 128, :])
    work[...] = jnp.concatenate(parts, axis=0) - less


def projected(k, foot, picked, pairs):
    return pl.pallas_call(
        functools.partial(again_kernel, k),
        in_specs=[VM] * 3,
        out_specs=[VM] * 2,
        out_shape=[like(128, 128), like(8, 128)],
        compiler_params=PARAMS,
        cost_estimate=cost(16 * 16 * 256 * 128),
        name="projected",
    )(foot, picked, resident(pairs))


def far_kernel(place, w0, w1, w2, w3, c0, c1, c2, c3, other, both, curv, work):
    for k, part in enumerate((w0, w1, w2, w3)):
        work[k * 128 : (k + 1) * 128, :] = part[...]
    scatter_far(place, work, [c[:1, :] for c in (c0, c1, c2, c3)], other, both, curv)


def scatter_other(place, works, curvs):
    return pl.pallas_call(
        far_kernel,
        in_specs=[VM] * 9,
        out_specs=[VM] * 3,
        out_shape=FAR_OUT,
        scratch_shapes=[SLOTS_BY_FRAMES],
        compiler_params=PARAMS,
        name="scatter_other",
    )(place, *works, *curvs)


def last_kernel(f0, f1, f2, f3, new):
    x = lax.axis_index("ta")
    for k, foot in enumerate((f0, f1, f2, f3)):
        new[rows_of(x ^ k), :] = foot[...]


def last(feet):
    return pl.pallas_call(
        last_kernel,
        in_specs=[VM] * 4,
        out_specs=VM,
        out_shape=like(512, TILE),
        compiler_params=PARAMS,
        name="last",
    )(*feet)


def swapped(x, axis, bits):
    n = lax.axis_size(axis)
    return lax.ppermute(x, axis, [(i, i ^ bits) for i in range(n)])


def across(x):
    return swapped(x, ("zh", "zl"), 7)


def summed_blocks(place, other, both, curv):
    came = swapped(other, "c", 1)
    ys = fold_core(scatter_mine(place, both, curv), came)
    zs = fold_y([ys[0]] + [swapped(ys[k], "y", k) for k in (3, 2, 1)])
    own = fold_z([zs[0]] + [swapped(zs[k], "zl", k) for k in (3, 2, 1)])
    return own, across(own)


def gathered(part, axis):
    near = [swapped(part, axis, k) for k in (1, 2, 3)]
    return jnp.concatenate([part] + near, axis=0)


def new_feet(column, near, far, foot, valid, pairs):
    picked, piece = picked_gradient(2, column, pick_near(column, near), far, foot, pairs)
    came = {2: swapped(piece, "ta", 2)}
    for k in (1, 3):
        piece = gradient(k, picked, foot, pairs)
        came[k] = swapped(piece, "ta", k)
    came[0] = gradient(0, picked, foot, pairs)
    own = stepped([came[k] for k in range(NGROUP)], foot, valid)
    return [own] + [swapped(own, "ta", k) for k in (1, 2, 3)], picked


def local(movie, traces, entry_comp, footprints):
    entry = entry_comp.reshape(NGROUP, 1, 128)
    twin, entry = lax.optimization_barrier((across(traces), entry))
    own = jnp.concatenate([traces, twin], axis=0)
    part = gathered(own, "zl")
    made = first(entry, movie, footprints.reshape(-1, TILE))
    part, place, column, valid, foot, pairs, proj, gram = lax.optimization_barrier(
        (part, *made)
    )
    near = gathered(part, "y")
    far = swapped(near, "c", 1)
    sums = numerators(place, column, proj, gram, pick_near(column, near), far)
    for step in range(ITERS):
        own = update(*summed_blocks(place, *sums), own)
        near = gathered(gathered(own, "zl"), "y")
        far = swapped(near, "c", 1)
        feet, picked = new_feet(column, near, far, foot, valid, pairs)
        if step + 1 < ITERS:
            works, curvs = zip(*(projected(k, feet[k], picked, pairs) for k in range(NGROUP)))
            sums = scatter_other(place, works, curvs)
            foot = jnp.concatenate(feet, axis=0)
    return own[:32], last(feet).reshape(footprints.shape)


def solution(mesh):
    torus = Mesh(
        mesh.devices.reshape(2, 4, 2, mesh.shape["gy"], mesh.shape["ta"]),
        ("zh", "y", "c", "zl", "ta"),
    )
    in_specs = (P(BLOCKS, "ta"), P(BLOCKS, "ta"), P(BLOCKS, None), P(BLOCKS, None, None))
    out_specs = (P(BLOCKS, "ta"), P(BLOCKS, None, None))
    return jax.shard_map(local, mesh=torus, in_specs=in_specs, out_specs=out_specs, check_vma=False)
```

```python
import functools

import jax
import jax.numpy as jnp
from jax import lax
from jax.experimental import pallas as pl
from jax.experimental.pallas import tpu as pltpu
from jax.sharding import Mesh
from jax.sharding import PartitionSpec as P


K = 2048
TILE = 128
SLOTS = 8
ITERS = 2
RIDGE = 1.0
BLOCKS = ("zh", "y", "c", "zl")
NGROUP = 4
GT = 16
HALF = 1024
NBLK = 16
ROWS = 72
WIDE = 264

VM = pl.BlockSpec(memory_space=pltpu.VMEM)
HB = pl.BlockSpec(memory_space=pltpu.HBM)
PARAMS = pltpu.CompilerParams(vmem_limit_bytes=24 * 1024 * 1024)
f32 = jnp.float32
bf16 = jnp.bfloat16


def like(*shape, dtype=f32):
    return jax.ShapeDtypeStruct(shape, dtype)


def cost(macs):
    return pl.CostEstimate(flops=2 * macs, bytes_accessed=1 << 20, transcendentals=0)


def split(x):
    hi = x.astype(bf16)
    lo = (x - hi.astype(f32)).astype(bf16)
    return hi, lo


def nt(a, b):
    return lax.dot_general(a, b, (((1,), (1,)), ((), ())), preferred_element_type=f32)


def nn(a, b):
    return lax.dot_general(a, b, (((1,), (0,)), ((), ())), preferred_element_type=f32)


def nt3(a, b):
    ah, al = split(a)
    bh, bl = split(b)
    return nt(ah, bh) + (nt(ah, bl) + nt(al, bh))


def nn3(a, b):
    ah, al = split(a)
    bh, bl = split(b)
    return nn(ah, bh) + (nn(ah, bl) + nn(al, bh))


def same_tile():
    i = lax.broadcasted_iota(jnp.int32, (128, 128), 0) // SLOTS
    j = lax.broadcasted_iota(jnp.int32, (128, 128), 1) // SLOTS
    return i == j


def stacked(x):
    hi = x.astype(bf16).astype(f32)
    return jnp.concatenate([hi, x - hi], axis=0).astype(bf16)


def as_column(row, n):
    i = lax.broadcasted_iota(jnp.int32, (n, n), 0)
    j = lax.broadcasted_iota(jnp.int32, (n, n), 1)
    return jnp.sum(jnp.where(i == j, row, 0.0), axis=1, keepdims=True)


def project(foot, pair):
    two = stacked(foot)
    out = nn(jnp.concatenate([two, two], axis=1), pair)
    return out[:SLOTS] + out[SLOTS:]


def correlate(picked, pair):
    out = nt(stacked(picked), pair)
    out = out[:SLOTS] + out[SLOTS:]
    return out[:, :TILE] + out[:, TILE:]


def rows_of(g):
    return pl.ds(pl.multiple_of(g * 128, 128), 128)


def prepare_kernel(entry, footprints, place, column, valid, foot, got):
    zh, y, c, zl = (lax.axis_index(name) for name in BLOCKS)
    x = lax.axis_index("ta")
    copies = []
    for k in range(NGROUP):
        at = pl.ds(pl.multiple_of((x ^ k) * 128, 128), 128)
        copies.append(
            pltpu.make_async_copy(footprints.at[at], foot.at[pl.ds(k * 128, 128)], got.at[k])
        )
        copies[-1].start()
    for k in range(NGROUP):
        s = slice(k * 128, (k + 1) * 128)
        comp = entry[x ^ k]
        owner = comp >> 5
        ozh, oy, oc, ozl = owner >> 5, (owner >> 3) & 3, (owner >> 2) & 1, owner & 3
        row = ((oc ^ c) * 4 + (oy ^ y)) * 256 + (comp & 31)
        index = row + (ozl ^ (3 * ozh) ^ zl ^ (3 * zh)) * 64 + (ozh ^ zh) * 32
        index = jnp.where(comp < K, index, K)
        place[:, s] = index
        at = as_column(index.astype(f32), 128)
        column[s, :] = at.astype(jnp.int32)
        valid[s, :] = jnp.where(at < K, 1.0, 0.0)
    for k in range(NGROUP):
        s = slice(k * 128, (k + 1) * 128)
        copies[k].wait()
        foot[s, :] = foot[s, :] * valid[s, :]


def prepare(entry, footprints):
    return pl.pallas_call(
        prepare_kernel,
        in_specs=[VM, HB],
        out_specs=[VM] * 4,
        out_shape=[
            like(1, 512, dtype=jnp.int32),
            like(512, 1, dtype=jnp.int32),
            like(512, 1),
            like(512, TILE),
        ],
        scratch_shapes=[pltpu.SemaphoreType.DMA((NGROUP,))],
        compiler_params=PARAMS,
        cost_estimate=cost(16 * 16 * 256 * 128),
        name="prepare",
    )(entry, pltpu.with_memory_space_constraint(footprints, pltpu.HBM))


def first_kernel(movie, foot, pairs, proj, gram, frames, came):
    x = lax.axis_index("ta")
    tall = GT * TILE
    for k in range(NGROUP):
        at = pl.ds(pl.multiple_of((x ^ k) * tall, tall), tall)
        pltpu.make_async_copy(movie.at[at], frames.at[pl.ds(k * tall, tall)], came.at[k]).start()

    def group(k, carry):
        s = rows_of(k)
        f = foot[s, :]
        gram[k] = jnp.where(same_tile(), nt3(f, f), 0.0)
        at = pl.ds(pl.multiple_of(k * tall, tall), tall)
        pltpu.make_async_copy(movie.at[at], frames.at[at], came.at[k]).wait()
        parts = []
        for t in range(GT):
            at = pl.ds(pl.multiple_of((k * GT + t) * TILE, TILE), TILE)
            hi, lo = split(frames[at, :])
            pair = jnp.concatenate([hi, lo], axis=0)
            pairs[k * GT + t] = pair
            parts.append(project(f[t * SLOTS : (t + 1) * SLOTS], pair))
        proj[s, :] = jnp.concatenate(parts, axis=0)
        return carry

    lax.fori_loop(0, NGROUP, group, 0)


def first(movie, foot):
    return pl.pallas_call(
        first_kernel,
        in_specs=[HB, VM],
        out_specs=[VM] * 3,
        out_shape=[
            pltpu.VMEM((64, 2 * TILE, 128), bf16),
            like(512, 128),
            like(NGROUP, 128, 128),
        ],
        scratch_shapes=[pltpu.VMEM((64 * TILE, 128), f32), pltpu.SemaphoreType.DMA((NGROUP,))],
        compiler_params=PARAMS,
        cost_estimate=cost(64 * 16 * 256 * 128),
        name="first",
    )(pltpu.with_memory_space_constraint(movie, pltpu.HBM), foot)


def scatter(half, place, both, curv, out, looped):
    n = place.shape[1]
    lane = lax.broadcasted_iota(jnp.int32, (256, n), 0)
    inside = jnp.where(lane[:128] == place % 64, 1.0, 0.0).astype(bf16)
    block = lax.broadcasted_iota(jnp.int32, (NBLK, n), 0) + half * NBLK
    ch, cl = split(jnp.where(block == place // 64, curv, 0.0))
    den = nt(ch, inside) + nt(cl, inside)
    dens = jnp.concatenate([den, jnp.zeros((8, 128), f32)], axis=0)
    for k in range(4):
        out[k, 256:, :] = dens[k * 4 : k * 4 + 8]

    def rows(k, carry):
        hot = jnp.where(lane + (half * HALF + k * 256) == place, 1.0, 0.0).astype(bf16)
        got = nn(hot, both[...])
        out[k, :256, :] = got[:, :128] + got[:, 128:]
        return carry

    if looped:
        lax.fori_loop(0, 4, rows, 0)
    else:
        for k in range(4):
            rows(k, 0)


def picked_from_far(column, far, near, out):
    both = jnp.concatenate(split(far[...]), axis=1)
    at = column[...]
    lane = lax.broadcasted_iota(jnp.int32, (at.shape[0], HALF), 1) + HALF
    got = nn(jnp.where(lane == at, 1.0, 0.0).astype(bf16), both)
    out[...] = got[:, :128] + got[:, 128:] + near[...]


def near_kernel(column, near, out):
    both = jnp.concatenate(split(near[...]), axis=1)
    lane = lax.broadcasted_iota(jnp.int32, (256, HALF), 1)

    def some(i, carry):
        s = pl.ds(pl.multiple_of(i * 256, 256), 256)
        hot = jnp.where(lane == column[s, :], 1.0, 0.0).astype(bf16)
        got = nn(hot, both)
        out[s, :] = got[:, :128] + got[:, 128:]
        return carry

    lax.fori_loop(0, 2, some, 0)


def pick_near(column, near):
    return pl.pallas_call(
        near_kernel,
        in_specs=[VM] * 2,
        out_specs=VM,
        out_shape=like(512, 128),
        compiler_params=PARAMS,
        cost_estimate=cost(512 * HALF * 256),
        name="pick_near",
    )(column, near)


SLOTS_BY_FRAMES = pltpu.VMEM((512, 128), f32)
FAR_OUT = [like(4, WIDE, 128), like(512, 256, dtype=bf16), like(8, 512)]


def scatter_far(place, work, rows, other, both, curv):
    two = jnp.concatenate(split(work[...]), axis=1)
    row = jnp.concatenate(rows, axis=1)
    both[...] = two
    curv[...] = jnp.broadcast_to(row, (8, 512))
    scatter(1, place[...], two, row, other, False)


def numer_kernel(place, column, proj, gram, got, far, other, both, curv, work):
    picked_from_far(column, far, got, work)
    rows = []
    for g in range(NGROUP):
        s = slice(g * 128, (g + 1) * 128)
        work[s, :] = proj[s, :] - nn3(gram[g], work[s, :])
        rows.append(jnp.sum(gram[g], axis=0, keepdims=True))
    scatter_far(place, work, rows, other, both, curv)


def numerators(place, column, proj, gram, got, far):
    return pl.pallas_call(
        numer_kernel,
        in_specs=[VM] * 6,
        out_specs=[VM] * 3,
        out_shape=FAR_OUT,
        scratch_shapes=[SLOTS_BY_FRAMES],
        compiler_params=PARAMS,
        name="numerators",
    )(place, column, proj, gram, got, far)


def mine_kernel(place, both, curv, mine):
    scatter(0, place[...], both, curv[:1, :], mine, True)


def scatter_mine(place, both, curv):
    return pl.pallas_call(
        mine_kernel,
        in_specs=[VM] * 3,
        out_specs=VM,
        out_shape=like(4, WIDE, 128),
        compiler_params=PARAMS,
        cost_estimate=cost(512 * HALF * 256),
        name="scatter_mine",
    )(place, both, curv)


def fold_core_kernel(mine, came, *outs):
    for k in range(4):
        outs[k][...] = mine[k] + came[k]


def fold_core(mine, came):
    return pl.pallas_call(
        fold_core_kernel,
        in_specs=[VM] * 2,
        out_specs=[VM] * 4,
        out_shape=[like(WIDE, 128)] * 4,
        compiler_params=PARAMS,
        name="fold_core",
    )(mine, came)


def fold_y_kernel(a, b, c, d, *outs):
    den = (a[256:, :] + b[256:, :]) + (c[256:, :] + d[256:, :])
    for k in range(4):
        s = slice(k * 64, (k + 1) * 64)
        outs[k][:64, :] = (a[s, :] + b[s, :]) + (c[s, :] + d[s, :])
        outs[k][64:, :] = jnp.broadcast_to(den[k : k + 1], (8, 128))


def fold_y(parts):
    return pl.pallas_call(
        fold_y_kernel,
        in_specs=[VM] * 4,
        out_specs=[VM] * 4,
        out_shape=[like(ROWS, 128)] * 4,
        compiler_params=PARAMS,
        name="fold_y",
    )(*parts)


def fold_z_kernel(a, b, c, d, out):
    out[...] = (a[...] + b[...]) + (c[...] + d[...])


def fold_z(parts):
    return pl.pallas_call(
        fold_z_kernel,
        in_specs=[VM] * 4,
        out_specs=VM,
        out_shape=like(ROWS, 128),
        compiler_params=PARAMS,
        name="fold_z",
    )(*parts)


def update_kernel(own, came, traces, out):
    a = as_column(own[64:65, :], 128)
    b = as_column(came[64:65, :], 128)
    for h in range(2):
        s = slice(h * 32, (h + 1) * 32)
        o = slice((1 - h) * 32, (2 - h) * 32)
        den = a[s] + b[o] + RIDGE
        out[s, :] = jnp.maximum(traces[s, :] + (own[s, :] + came[o, :]) / den, 0.0)


def update(own, came, traces):
    return pl.pallas_call(
        update_kernel,
        in_specs=[VM] * 3,
        out_specs=VM,
        out_shape=like(64, 128),
        compiler_params=PARAMS,
        name="update",
    )(own, came, traces)


def resident(pairs):
    return pltpu.with_memory_space_constraint(pairs, pltpu.VMEM)


def grad_piece(k, picked, foot, pairs, out):
    p = picked[k * 128 : (k + 1) * 128, :]
    gram = jnp.where(same_tile(), nt3(p, p), 0.0)
    out[128:, :] = jnp.broadcast_to(jnp.sum(gram, axis=0, keepdims=True), (8, 128))
    parts = []
    for t in range(GT):
        parts.append(correlate(p[t * SLOTS : (t + 1) * SLOTS], pairs[k * GT + t]))
    less = nn3(gram, foot[k * 128 : (k + 1) * 128, :])
    out[:128, :] = jnp.concatenate(parts, axis=0) - less


def picked_grad_kernel(k, column, got, far, foot, pairs, picked, out):
    picked_from_far(column, far, got, picked)
    grad_piece(k, picked, foot, pairs, out)


def picked_gradient(k, column, got, far, foot, pairs):
    return pl.pallas_call(
        functools.partial(picked_grad_kernel, k),
        in_specs=[VM] * 5,
        out_specs=[VM] * 2,
        out_shape=[like(512, 128), like(136, 128)],
        compiler_params=PARAMS,
        cost_estimate=cost(512 * HALF * 256),
        name="picked_gradient",
    )(column, got, far, foot, resident(pairs))


def grad_kernel(k, picked, foot, pairs, out):
    grad_piece(k, picked, foot, pairs, out)


def gradient(k, picked, foot, pairs):
    return pl.pallas_call(
        functools.partial(grad_kernel, k),
        in_specs=[VM] * 3,
        out_specs=VM,
        out_shape=like(136, 128),
        compiler_params=PARAMS,
        cost_estimate=cost(16 * 16 * 256 * 128),
        name="gradient",
    )(picked, foot, resident(pairs))


def step_kernel(a, b, c, d, foot, valid, new):
    total = (a[...] + c[...]) + (b[...] + d[...])
    dsp = as_column(total[128:129, :], 128) + RIDGE
    new[...] = jnp.maximum(foot[:128, :] + total[:128] / dsp, 0.0) * valid[:128, :]


def stepped(parts, foot, valid):
    return pl.pallas_call(
        step_kernel,
        in_specs=[VM] * 6,
        out_specs=VM,
        out_shape=like(128, TILE),
        compiler_params=PARAMS,
        name="step",
    )(*parts, foot, valid)


def again_kernel(k, foot, picked, pairs, work, curv):
    f = foot[...]
    gram = jnp.where(same_tile(), nt3(f, f), 0.0)
    curv[...] = jnp.broadcast_to(jnp.sum(gram, axis=0, keepdims=True), (8, 128))
    parts = []
    for t in range(GT):
        parts.append(project(f[t * SLOTS : (t + 1) * SLOTS], pairs[k * GT + t]))
    less = nn3(gram, picked[k * 128 : (k + 1) * 128, :])
    work[...] = jnp.concatenate(parts, axis=0) - less


def projected(k, foot, picked, pairs):
    return pl.pallas_call(
        functools.partial(again_kernel, k),
        in_specs=[VM] * 3,
        out_specs=[VM] * 2,
        out_shape=[like(128, 128), like(8, 128)],
        compiler_params=PARAMS,
        cost_estimate=cost(16 * 16 * 256 * 128),
        name="projected",
    )(foot, picked, resident(pairs))


def far_kernel(place, w0, w1, w2, w3, c0, c1, c2, c3, other, both, curv, work):
    for k, part in enumerate((w0, w1, w2, w3)):
        work[k * 128 : (k + 1) * 128, :] = part[...]
    scatter_far(place, work, [c[:1, :] for c in (c0, c1, c2, c3)], other, both, curv)


def scatter_other(place, works, curvs):
    return pl.pallas_call(
        far_kernel,
        in_specs=[VM] * 9,
        out_specs=[VM] * 3,
        out_shape=FAR_OUT,
        scratch_shapes=[SLOTS_BY_FRAMES],
        compiler_params=PARAMS,
        name="scatter_other",
    )(place, *works, *curvs)


def last_kernel(f0, f1, f2, f3, new):
    x = lax.axis_index("ta")
    for k, foot in enumerate((f0, f1, f2, f3)):
        new[rows_of(x ^ k), :] = foot[...]


def last(feet):
    return pl.pallas_call(
        last_kernel,
        in_specs=[VM] * 4,
        out_specs=VM,
        out_shape=like(512, TILE),
        compiler_params=PARAMS,
        name="last",
    )(*feet)


def swapped(x, axis, bits):
    n = lax.axis_size(axis)
    return lax.ppermute(x, axis, [(i, i ^ bits) for i in range(n)])


def across(x):
    return swapped(x, ("zh", "zl"), 7)


def summed_blocks(place, other, both, curv):
    came = swapped(other, "c", 1)
    ys = fold_core(scatter_mine(place, both, curv), came)
    zs = fold_y([ys[0]] + [swapped(ys[k], "y", k) for k in (3, 2, 1)])
    own = fold_z([zs[0]] + [swapped(zs[k], "zl", k) for k in (3, 2, 1)])
    return own, across(own)


def gathered(part, axis):
    near = [swapped(part, axis, k) for k in (1, 2, 3)]
    return jnp.concatenate([part] + near, axis=0)


def new_feet(column, near, far, foot, valid, pairs):
    picked, piece = picked_gradient(3, column, pick_near(column, near), far, foot, pairs)
    came = {3: swapped(piece, "ta", 3)}
    for k in (2, 1):
        piece = gradient(k, picked, foot, pairs)
        came[k] = swapped(piece, "ta", k)
    came[0] = gradient(0, picked, foot, pairs)
    own = stepped([came[k] for k in range(NGROUP)], foot, valid)
    return [own] + [swapped(own, "ta", k) for k in (1, 2, 3)], picked


def local(movie, traces, entry_comp, footprints):
    entry = entry_comp.reshape(NGROUP, 1, 128)
    twin, entry = lax.optimization_barrier((across(traces), entry))
    own = jnp.concatenate([traces, twin], axis=0)
    part = gathered(own, "zl")
    made = prepare(entry, footprints.reshape(-1, TILE))
    part, place, column, valid, foot = lax.optimization_barrier((part, *made))
    near = gathered(part, "y")
    made = first(movie, foot)
    near, pairs, proj, gram = lax.optimization_barrier((near, *made))
    far = swapped(near, "c", 1)
    sums = numerators(place, column, proj, gram, pick_near(column, near), far)
    for step in range(ITERS):
        own = update(*summed_blocks(place, *sums), own)
        near = gathered(gathered(own, "zl"), "y")
        far = swapped(near, "c", 1)
        feet, picked = new_feet(column, near, far, foot, valid, pairs)
        if step + 1 < ITERS:
            works, curvs = zip(*(projected(k, feet[k], picked, pairs) for k in range(NGROUP)))
            sums = scatter_other(place, works, curvs)
            foot = jnp.concatenate(feet, axis=0)
    return own[:32], last(feet).reshape(footprints.shape)


def solution(mesh):
    torus = Mesh(
        mesh.devices.reshape(2, 4, 2, mesh.shape["gy"], mesh.shape["ta"]),
        ("zh", "y", "c", "zl", "ta"),
    )
    in_specs = (P(BLOCKS, "ta"), P(BLOCKS, "ta"), P(BLOCKS, None), P(BLOCKS, None, None))
    out_specs = (P(BLOCKS, "ta"), P(BLOCKS, None, None))
    return jax.shard_map(local, mesh=torus, in_specs=in_specs, out_specs=out_specs, check_vma=False)
```

```python
import functools

import jax
import jax.numpy as jnp
from jax import lax
from jax.experimental import pallas as pl
from jax.experimental.pallas import tpu as pltpu
from jax.sharding import Mesh
from jax.sharding import PartitionSpec as P


K = 2048
TILE = 128
SLOTS = 8
ITERS = 2
RIDGE = 1.0
BLOCKS = ("zh", "y", "c", "zl")
NGROUP = 4
GT = 16
HALF = 1024
NBLK = 16
ROWS = 72
WIDE = 264

VM = pl.BlockSpec(memory_space=pltpu.VMEM)
HB = pl.BlockSpec(memory_space=pltpu.HBM)
PARAMS = pltpu.CompilerParams(vmem_limit_bytes=24 * 1024 * 1024)
f32 = jnp.float32
bf16 = jnp.bfloat16


def like(*shape, dtype=f32):
    return jax.ShapeDtypeStruct(shape, dtype)


def cost(macs):
    return pl.CostEstimate(flops=2 * macs, bytes_accessed=1 << 20, transcendentals=0)


def split(x):
    hi = x.astype(bf16)
    lo = (x - hi.astype(f32)).astype(bf16)
    return hi, lo


def nt(a, b):
    return lax.dot_general(a, b, (((1,), (1,)), ((), ())), preferred_element_type=f32)


def nn(a, b):
    return lax.dot_general(a, b, (((1,), (0,)), ((), ())), preferred_element_type=f32)


def nt3(a, b):
    ah, al = split(a)
    bh, bl = split(b)
    return nt(ah, bh) + (nt(ah, bl) + nt(al, bh))


def nn3(a, b):
    ah, al = split(a)
    bh, bl = split(b)
    return nn(ah, bh) + (nn(ah, bl) + nn(al, bh))


def same_tile():
    i = lax.broadcasted_iota(jnp.int32, (128, 128), 0) // SLOTS
    j = lax.broadcasted_iota(jnp.int32, (128, 128), 1) // SLOTS
    return i == j


def stacked(x):
    hi = x.astype(bf16).astype(f32)
    return jnp.concatenate([hi, x - hi], axis=0).astype(bf16)


def as_column(row, n):
    i = lax.broadcasted_iota(jnp.int32, (n, n), 0)
    j = lax.broadcasted_iota(jnp.int32, (n, n), 1)
    return jnp.sum(jnp.where(i == j, row, 0.0), axis=1, keepdims=True)


def project(foot, pair):
    two = stacked(foot)
    out = nn(jnp.concatenate([two, two], axis=1), pair)
    return out[:SLOTS] + out[SLOTS:]


def correlate(picked, pair):
    out = nt(stacked(picked), pair)
    out = out[:SLOTS] + out[SLOTS:]
    return out[:, :TILE] + out[:, TILE:]


def rows_of(g):
    return pl.ds(pl.multiple_of(g * 128, 128), 128)


def prepare_kernel(entry, footprints, place, column, valid, foot, got):
    zh, y, c, zl = (lax.axis_index(name) for name in BLOCKS)
    x = lax.axis_index("ta")
    copies = []
    for k in range(NGROUP):
        at = pl.ds(pl.multiple_of((x ^ k) * 128, 128), 128)
        copies.append(
            pltpu.make_async_copy(footprints.at[at], foot.at[pl.ds(k * 128, 128)], got.at[k])
        )
        copies[-1].start()
    for k in range(NGROUP):
        s = slice(k * 128, (k + 1) * 128)
        comp = entry[x ^ k]
        owner = comp >> 5
        ozh, oy, oc, ozl = owner >> 5, (owner >> 3) & 3, (owner >> 2) & 1, owner & 3
        row = ((oc ^ c) * 4 + (oy ^ y)) * 256 + (comp & 31)
        index = row + (ozl ^ (3 * ozh) ^ zl ^ (3 * zh)) * 64 + (ozh ^ zh) * 32
        index = jnp.where(comp < K, index, K)
        place[:, s] = index
        at = as_column(index.astype(f32), 128)
        column[s, :] = at.astype(jnp.int32)
        valid[s, :] = jnp.where(at < K, 1.0, 0.0)
    for k in range(NGROUP):
        s = slice(k * 128, (k + 1) * 128)
        copies[k].wait()
        foot[s, :] = foot[s, :] * valid[s, :]


def prepare(entry, footprints):
    return pl.pallas_call(
        prepare_kernel,
        in_specs=[VM, HB],
        out_specs=[VM] * 4,
        out_shape=[
            like(1, 512, dtype=jnp.int32),
            like(512, 1, dtype=jnp.int32),
            like(512, 1),
            like(512, TILE),
        ],
        scratch_shapes=[pltpu.SemaphoreType.DMA((NGROUP,))],
        compiler_params=PARAMS,
        cost_estimate=cost(16 * 16 * 256 * 128),
        name="prepare",
    )(entry, pltpu.with_memory_space_constraint(footprints, pltpu.HBM))


def first_kernel(movie, foot, pairs, proj, gram, frames, came):
    x = lax.axis_index("ta")
    tall = GT * TILE
    for k in range(NGROUP):
        at = pl.ds(pl.multiple_of((x ^ k) * tall, tall), tall)
        pltpu.make_async_copy(movie.at[at], frames.at[pl.ds(k * tall, tall)], came.at[k]).start()

    def group(k, carry):
        s = rows_of(k)
        f = foot[s, :]
        gram[k] = jnp.where(same_tile(), nt3(f, f), 0.0)
        at = pl.ds(pl.multiple_of(k * tall, tall), tall)
        pltpu.make_async_copy(movie.at[at], frames.at[at], came.at[k]).wait()
        parts = []
        for t in range(GT):
            at = pl.ds(pl.multiple_of((k * GT + t) * TILE, TILE), TILE)
            hi, lo = split(frames[at, :])
            pair = jnp.concatenate([hi, lo], axis=0)
            pairs[k * GT + t] = pair
            parts.append(project(f[t * SLOTS : (t + 1) * SLOTS], pair))
        proj[s, :] = jnp.concatenate(parts, axis=0)
        return carry

    lax.fori_loop(0, NGROUP, group, 0)


def first(movie, foot):
    return pl.pallas_call(
        first_kernel,
        in_specs=[HB, VM],
        out_specs=[VM] * 3,
        out_shape=[
            pltpu.VMEM((64, 2 * TILE, 128), bf16),
            like(512, 128),
            like(NGROUP, 128, 128),
        ],
        scratch_shapes=[pltpu.VMEM((64 * TILE, 128), f32), pltpu.SemaphoreType.DMA((NGROUP,))],
        compiler_params=PARAMS,
        cost_estimate=cost(64 * 16 * 256 * 128),
        name="first",
    )(pltpu.with_memory_space_constraint(movie, pltpu.HBM), foot)


def scatter(half, place, both, curv, out, looped):
    n = place.shape[1]
    lane = lax.broadcasted_iota(jnp.int32, (256, n), 0)
    inside = jnp.where(lane[:128] == place % 64, 1.0, 0.0).astype(bf16)
    block = lax.broadcasted_iota(jnp.int32, (NBLK, n), 0) + half * NBLK
    ch, cl = split(jnp.where(block == place // 64, curv, 0.0))
    den = nt(ch, inside) + nt(cl, inside)
    dens = jnp.concatenate([den, jnp.zeros((8, 128), f32)], axis=0)
    for k in range(4):
        out[k, 256:, :] = dens[k * 4 : k * 4 + 8]

    def rows(k, carry):
        hot = jnp.where(lane + (half * HALF + k * 256) == place, 1.0, 0.0).astype(bf16)
        got = nn(hot, both[...])
        out[k, :256, :] = got[:, :128] + got[:, 128:]
        return carry

    if looped:
        lax.fori_loop(0, 4, rows, 0)
    else:
        for k in range(4):
            rows(k, 0)


def picked_from_far(column, far, near, out):
    both = jnp.concatenate(split(far[...]), axis=1)
    at = column[...]
    lane = lax.broadcasted_iota(jnp.int32, (at.shape[0], HALF), 1) + HALF
    got = nn(jnp.where(lane == at, 1.0, 0.0).astype(bf16), both)
    out[...] = got[:, :128] + got[:, 128:] + near[...]


def near_kernel(column, near, out):
    both = jnp.concatenate(split(near[...]), axis=1)
    lane = lax.broadcasted_iota(jnp.int32, (256, HALF), 1)

    def some(i, carry):
        s = pl.ds(pl.multiple_of(i * 256, 256), 256)
        hot = jnp.where(lane == column[s, :], 1.0, 0.0).astype(bf16)
        got = nn(hot, both)
        out[s, :] = got[:, :128] + got[:, 128:]
        return carry

    lax.fori_loop(0, 2, some, 0)


def pick_near(column, near):
    return pl.pallas_call(
        near_kernel,
        in_specs=[VM] * 2,
        out_specs=VM,
        out_shape=like(512, 128),
        compiler_params=PARAMS,
        cost_estimate=cost(512 * HALF * 256),
        name="pick_near",
    )(column, near)


SLOTS_BY_FRAMES = pltpu.VMEM((512, 128), f32)
FAR_OUT = [like(4, WIDE, 128), like(512, 256, dtype=bf16), like(8, 512)]


def scatter_far(place, work, rows, other, both, curv):
    two = jnp.concatenate(split(work[...]), axis=1)
    row = jnp.concatenate(rows, axis=1)
    both[...] = two
    curv[...] = jnp.broadcast_to(row, (8, 512))
    scatter(1, place[...], two, row, other, False)


def numer_kernel(place, column, proj, gram, got, far, other, both, curv, work):
    picked_from_far(column, far, got, work)
    rows = []
    for g in range(NGROUP):
        s = slice(g * 128, (g + 1) * 128)
        work[s, :] = proj[s, :] - nn3(gram[g], work[s, :])
        rows.append(jnp.sum(gram[g], axis=0, keepdims=True))
    scatter_far(place, work, rows, other, both, curv)


def numerators(place, column, proj, gram, got, far):
    return pl.pallas_call(
        numer_kernel,
        in_specs=[VM] * 6,
        out_specs=[VM] * 3,
        out_shape=FAR_OUT,
        scratch_shapes=[SLOTS_BY_FRAMES],
        compiler_params=PARAMS,
        name="numerators",
    )(place, column, proj, gram, got, far)


def mine_kernel(place, both, curv, mine):
    scatter(0, place[...], both, curv[:1, :], mine, True)


def scatter_mine(place, both, curv):
    return pl.pallas_call(
        mine_kernel,
        in_specs=[VM] * 3,
        out_specs=VM,
        out_shape=like(4, WIDE, 128),
        compiler_params=PARAMS,
        cost_estimate=cost(512 * HALF * 256),
        name="scatter_mine",
    )(place, both, curv)


def fold_core_kernel(mine, came, *outs):
    for k in range(4):
        outs[k][...] = mine[k] + came[k]


def fold_core(mine, came):
    return pl.pallas_call(
        fold_core_kernel,
        in_specs=[VM] * 2,
        out_specs=[VM] * 4,
        out_shape=[like(WIDE, 128)] * 4,
        compiler_params=PARAMS,
        name="fold_core",
    )(mine, came)


def fold_y_kernel(a, b, c, d, *outs):
    den = (a[256:, :] + b[256:, :]) + (c[256:, :] + d[256:, :])
    for k in range(4):
        s = slice(k * 64, (k + 1) * 64)
        outs[k][:64, :] = (a[s, :] + b[s, :]) + (c[s, :] + d[s, :])
        outs[k][64:, :] = jnp.broadcast_to(den[k : k + 1], (8, 128))


def fold_y(parts):
    return pl.pallas_call(
        fold_y_kernel,
        in_specs=[VM] * 4,
        out_specs=[VM] * 4,
        out_shape=[like(ROWS, 128)] * 4,
        compiler_params=PARAMS,
        name="fold_y",
    )(*parts)


def fold_z_kernel(a, b, c, d, out):
    out[...] = (a[...] + b[...]) + (c[...] + d[...])


def fold_z(parts):
    return pl.pallas_call(
        fold_z_kernel,
        in_specs=[VM] * 4,
        out_specs=VM,
        out_shape=like(ROWS, 128),
        compiler_params=PARAMS,
        name="fold_z",
    )(*parts)


def update_kernel(own, came, traces, out):
    a = as_column(own[64:65, :], 128)
    b = as_column(came[64:65, :], 128)
    for h in range(2):
        s = slice(h * 32, (h + 1) * 32)
        o = slice((1 - h) * 32, (2 - h) * 32)
        den = a[s] + b[o] + RIDGE
        out[s, :] = jnp.maximum(traces[s, :] + (own[s, :] + came[o, :]) / den, 0.0)


def update(own, came, traces):
    return pl.pallas_call(
        update_kernel,
        in_specs=[VM] * 3,
        out_specs=VM,
        out_shape=like(64, 128),
        compiler_params=PARAMS,
        name="update",
    )(own, came, traces)


def resident(pairs):
    return pltpu.with_memory_space_constraint(pairs, pltpu.VMEM)


def grad_piece(k, picked, foot, pairs, out):
    p = picked[k * 128 : (k + 1) * 128, :]
    gram = jnp.where(same_tile(), nt3(p, p), 0.0)
    out[128:, :] = jnp.broadcast_to(jnp.sum(gram, axis=0, keepdims=True), (8, 128))
    parts = []
    for t in range(GT):
        parts.append(correlate(p[t * SLOTS : (t + 1) * SLOTS], pairs[k * GT + t]))
    less = nn3(gram, foot[k * 128 : (k + 1) * 128, :])
    out[:128, :] = jnp.concatenate(parts, axis=0) - less


def picked_grad_kernel(k, column, got, far, foot, pairs, picked, out):
    picked_from_far(column, far, got, picked)
    grad_piece(k, picked, foot, pairs, out)


def picked_gradient(k, column, got, far, foot, pairs):
    return pl.pallas_call(
        functools.partial(picked_grad_kernel, k),
        in_specs=[VM] * 5,
        out_specs=[VM] * 2,
        out_shape=[like(512, 128), like(136, 128)],
        compiler_params=PARAMS,
        cost_estimate=cost(512 * HALF * 256),
        name="picked_gradient",
    )(column, got, far, foot, resident(pairs))


def grad_kernel(k, picked, foot, pairs, out):
    grad_piece(k, picked, foot, pairs, out)


def gradient(k, picked, foot, pairs):
    return pl.pallas_call(
        functools.partial(grad_kernel, k),
        in_specs=[VM] * 3,
        out_specs=VM,
        out_shape=like(136, 128),
        compiler_params=PARAMS,
        cost_estimate=cost(16 * 16 * 256 * 128),
        name="gradient",
    )(picked, foot, resident(pairs))


def step_kernel(a, b, c, d, foot, valid, new):
    total = (a[...] + c[...]) + (b[...] + d[...])
    dsp = as_column(total[128:129, :], 128) + RIDGE
    new[...] = jnp.maximum(foot[:128, :] + total[:128] / dsp, 0.0) * valid[:128, :]


def stepped(parts, foot, valid):
    return pl.pallas_call(
        step_kernel,
        in_specs=[VM] * 6,
        out_specs=VM,
        out_shape=like(128, TILE),
        compiler_params=PARAMS,
        name="step",
    )(*parts, foot, valid)


def again_kernel(k, foot, picked, pairs, work, curv):
    f = foot[...]
    gram = jnp.where(same_tile(), nt3(f, f), 0.0)
    curv[...] = jnp.broadcast_to(jnp.sum(gram, axis=0, keepdims=True), (8, 128))
    parts = []
    for t in range(GT):
        parts.append(project(f[t * SLOTS : (t + 1) * SLOTS], pairs[k * GT + t]))
    less = nn3(gram, picked[k * 128 : (k + 1) * 128, :])
    work[...] = jnp.concatenate(parts, axis=0) - less


def projected(k, foot, picked, pairs):
    return pl.pallas_call(
        functools.partial(again_kernel, k),
        in_specs=[VM] * 3,
        out_specs=[VM] * 2,
        out_shape=[like(128, 128), like(8, 128)],
        compiler_params=PARAMS,
        cost_estimate=cost(16 * 16 * 256 * 128),
        name="projected",
    )(foot, picked, resident(pairs))


def far_kernel(place, w0, w1, w2, w3, c0, c1, c2, c3, other, both, curv, work):
    for k, part in enumerate((w0, w1, w2, w3)):
        work[k * 128 : (k + 1) * 128, :] = part[...]
    scatter_far(place, work, [c[:1, :] for c in (c0, c1, c2, c3)], other, both, curv)


def scatter_other(place, works, curvs):
    return pl.pallas_call(
        far_kernel,
        in_specs=[VM] * 9,
        out_specs=[VM] * 3,
        out_shape=FAR_OUT,
        scratch_shapes=[SLOTS_BY_FRAMES],
        compiler_params=PARAMS,
        name="scatter_other",
    )(place, *works, *curvs)


def last_kernel(f0, f1, f2, f3, new):
    x = lax.axis_index("ta")
    for k, foot in enumerate((f0, f1, f2, f3)):
        new[rows_of(x ^ k), :] = foot[...]


def last(feet):
    return pl.pallas_call(
        last_kernel,
        in_specs=[VM] * 4,
        out_specs=VM,
        out_shape=like(512, TILE),
        compiler_params=PARAMS,
        name="last",
    )(*feet)


def swapped(x, axis, bits):
    n = lax.axis_size(axis)
    return lax.ppermute(x, axis, [(i, i ^ bits) for i in range(n)])


def across(x):
    return swapped(x, ("zh", "zl"), 7)


def summed_blocks(place, other, both, curv):
    came = swapped(other, "c", 1)
    ys = fold_core(scatter_mine(place, both, curv), came)
    zs = fold_y([ys[0]] + [swapped(ys[k], "y", k) for k in (3, 2, 1)])
    own = fold_z([zs[0]] + [swapped(zs[k], "zl", k) for k in (2, 3, 1)])
    return own, across(own)


def gathered(part, axis):
    near = [swapped(part, axis, k) for k in (1, 2, 3)]
    return jnp.concatenate([part] + near, axis=0)


def new_feet(column, near, far, foot, valid, pairs):
    picked, piece = picked_gradient(3, column, pick_near(column, near), far, foot, pairs)
    came = {3: swapped(piece, "ta", 3)}
    for k in (2, 1):
        piece = gradient(k, picked, foot, pairs)
        came[k] = swapped(piece, "ta", k)
    came[0] = gradient(0, picked, foot, pairs)
    own = stepped([came[k] for k in range(NGROUP)], foot, valid)
    return [own] + [swapped(own, "ta", k) for k in (1, 2, 3)], picked


def local(movie, traces, entry_comp, footprints):
    entry = entry_comp.reshape(NGROUP, 1, 128)
    own = jnp.concatenate([traces, across(traces)], axis=0)
    part = gathered(own, "zl")
    made = prepare(entry, footprints.reshape(-1, TILE))
    part, place, column, valid, foot = lax.optimization_barrier((part, *made))
    near = gathered(part, "y")
    made = first(movie, foot)
    near, pairs, proj, gram = lax.optimization_barrier((near, *made))
    far = swapped(near, "c", 1)
    sums = numerators(place, column, proj, gram, pick_near(column, near), far)
    for step in range(ITERS):
        own = update(*summed_blocks(place, *sums), own)
        near = gathered(own, "zl")
        near = gathered(near, "y")
        far = swapped(near, "c", 1)
        feet, picked = new_feet(column, near, far, foot, valid, pairs)
        if step + 1 < ITERS:
            works, curvs = zip(*(projected(k, feet[k], picked, pairs) for k in range(NGROUP)))
            sums = scatter_other(place, works, curvs)
            foot = jnp.concatenate(feet, axis=0)
    return own[:32], last(feet).reshape(footprints.shape)


def solution(mesh):
    torus = Mesh(
        mesh.devices.reshape(2, 4, 2, mesh.shape["gy"], mesh.shape["ta"]),
        ("zh", "y", "c", "zl", "ta"),
    )
    in_specs = (P(BLOCKS, "ta"), P(BLOCKS, "ta"), P(BLOCKS, None), P(BLOCKS, None, None))
    out_specs = (P(BLOCKS, "ta"), P(BLOCKS, None, None))
    return jax.shard_map(local, mesh=torus, in_specs=in_specs, out_specs=out_specs, check_vma=False)
```
